128 devices in a mesh: batch: 1, rows: 128 (over z, y, x, core).
Axes of the slice: x: 4, y: 4, z: 4, core: 2. Of those that a mesh axis runs over, the one named last changes fastest.
Arguments:
- a_mat: float32 [524288, 512], P(('batch', 'rows'))
- rhs: float32 [524288, 128], P(('batch', 'rows'))
Outputs:
- output 1: float32 [512, 128], P('batch')
- output 2: float32 [512, 512], P('batch')
All inputs are finite; a program needn't handle non-finite values.
Results may differ from the reference program's by a relative error of at most 0.001.
Values sent between devices are 32-bit elements.
A program may use at most 1 GiB of HBM per device.

```python
import jax
import jax.numpy as jnp
from jax import lax
import math

M_ROWS = 524288
N_COLS = 512
N_RHS = 128
SHARDS = 128
COND_NUMBER = 1000.0
NOISE_LEVEL = 0.001


def setup_inputs(seed: int = 0, part: int = 0) -> dict:
    part_key = jax.random.fold_in(jax.random.key(seed), part)
    key_base, key_mix, key_sol, key_noise = jax.random.split(part_key, 4)
    rows_per = M_ROWS // SHARDS
    base = jax.random.normal(key_base, (M_ROWS, N_COLS), jnp.float32)
    row_shard = jnp.arange(M_ROWS) // rows_per
    col_owner = jnp.arange(N_COLS) % SHARDS
    low_weight = 0.5 / math.sqrt(SHARDS)
    weights = jnp.where(row_shard[:, None] == col_owner[None, :], 1.0, low_weight)
    col_scale = 1.0 / math.sqrt(rows_per * (1.0 + 0.25 * (SHARDS - 1) / SHARDS))
    basis = base * weights * col_scale
    ortho = jnp.linalg.qr(jax.random.normal(key_mix, (N_COLS, N_COLS), jnp.float32))[0]
    tail_len = N_COLS // 4
    tail_pos = jnp.clip((jnp.arange(N_COLS) - (N_COLS - tail_len)) / (tail_len - 1), 0.0, 1.0)
    sigma = jnp.power(COND_NUMBER, -tail_pos)
    upper_c = jnp.linalg.qr(sigma[:, None] * ortho.T)[1] * math.sqrt(N_COLS)
    a_mat = jnp.dot(basis, upper_c, precision=lax.Precision.HIGHEST)
    x_true = jax.random.normal(key_sol, (N_COLS, N_RHS), jnp.float32)
    signal = jnp.dot(a_mat, x_true, precision=lax.Precision.HIGHEST)
    noise_scale = NOISE_LEVEL * jnp.sqrt(jnp.mean(signal * signal))
    rhs = signal + noise_scale * jax.random.normal(key_noise, (M_ROWS, N_RHS), jnp.float32)
    return {"a_mat": a_mat.astype(jnp.float32), "rhs": rhs.astype(jnp.float32)}


def reference(a_mat, rhs):
    highest = lax.Precision.HIGHEST
    gram_one = jnp.dot(a_mat.T, a_mat, precision=highest, preferred_element_type=jnp.float32)
    low_one = jnp.linalg.cholesky(gram_one)
    q_one = lax.linalg.triangular_solve(low_one, a_mat, left_side=False, lower=True, transpose_a=True)
    gram_two = jnp.dot(q_one.T, q_one, precision=highest, preferred_element_type=jnp.float32)
    low_two = jnp.linalg.cholesky(gram_two)
    proj_one = jnp.dot(q_one.T, rhs, precision=highest, preferred_element_type=jnp.float32)
    proj_two = lax.linalg.triangular_solve(low_two, proj_one, left_side=True, lower=True)
    upper_r = jnp.dot(low_two.T, low_one.T, precision=highest, preferred_element_type=jnp.float32)
    x_sol = lax.linalg.triangular_solve(upper_r, proj_two, left_side=True, lower=False)
    return (x_sol, upper_r)
```

```python
import functools
import jax, jax.numpy as jnp
from jax import lax
from jax.experimental import pallas as pl
from jax.experimental.pallas import tpu as pltpu
from jax.sharding import PartitionSpec as P

HIGHEST = lax.Precision.HIGHEST
CHIPS = 64
CH = 16


def owner_index(chip, n_own):
    idx = (chip * n_own + CHIPS - 1) // CHIPS
    return idx, jnp.logical_and((idx * CHIPS) // n_own == chip, idx < n_own)


def sum_kernel(n_own, x_ref, o_ref, pair_buf, part, rs_buf, red, sems):
    dev = lax.axis_index("rows")
    chip, core = dev // 2, dev % 2
    half = n_own * CH
    mine = pl.multiple_of(core * half, CH)
    other = pl.multiple_of((1 - core) * half, CH)
    partner = {"rows": chip * 2 + 1 - core}

    def peer(step):
        t = (chip + step) % CHIPS
        return t, {"rows": t * 2 + core}

    barrier = pltpu.get_barrier_semaphore()
    pl.semaphore_signal(barrier, inc=1, device_id=partner)

    @pl.loop(1, CHIPS)
    def _(step):
        pl.semaphore_signal(barrier, inc=1, device_id=peer(step)[1])
    pl.semaphore_wait(barrier, CHIPS)

    pair = pltpu.make_async_remote_copy(x_ref.at[pl.ds(other, half)], pair_buf, sems.at[0], sems.at[1], device_id=partner)
    pair.start()
    pair.wait()
    part[...] = x_ref[pl.ds(mine, half), :] + pair_buf[...]

    my_idx, owner = owner_index(chip, n_own)
    my_row = pl.multiple_of(my_idx * CH, CH)

    @pl.loop(1, CHIPS)
    def _(step):
        t, dst = peer(step)
        idx, owns = owner_index(t, n_own)

        @pl.when(owns)
        def _():
            pltpu.make_async_remote_copy(part.at[pl.ds(pl.multiple_of(idx * CH, CH), CH)],
                                         rs_buf.at[pl.ds(pl.multiple_of((step - 1) * CH, CH), CH)],
                                         sems.at[2], sems.at[3], device_id=dst).start()

    def wait_rows(n, sem):
        pltpu.make_async_copy(part.at[pl.ds(0, n * CH)], part.at[pl.ds(0, n * CH)], sem).wait()

    @pl.when(owner)
    def _():
        pltpu.make_async_copy(rs_buf, rs_buf, sems.at[3]).wait()
        tot = part[pl.ds(my_row, CH), :]
        for s in range(CHIPS - 1):
            tot = tot + rs_buf[pl.ds(s * CH, CH), :]
        red[...] = tot
        o_ref[pl.ds(mine + my_row, CH), :] = tot

        @pl.loop(1, CHIPS)
        def _(step):
            pltpu.make_async_remote_copy(red, o_ref.at[pl.ds(pl.multiple_of(mine + my_row, CH), CH)],
                                         sems.at[4], sems.at[5], device_id=peer(step)[1]).start()
        wait_rows(n_own - 1, sems.at[2])
        wait_rows(n_own - 1, sems.at[5])

    @pl.when(jnp.logical_not(owner))
    def _():
        wait_rows(n_own, sems.at[2])
        wait_rows(n_own, sems.at[5])

    swap = pltpu.make_async_remote_copy(o_ref.at[pl.ds(mine, half)], o_ref.at[pl.ds(mine, half)], sems.at[6], sems.at[7], device_id=partner)
    swap.start()
    swap.wait()

    @pl.when(owner)
    def _():
        pltpu.make_async_copy(rs_buf, rs_buf, sems.at[4]).wait()


def sum_all(x, cid):
    rows = x.shape[0]
    half = rows // 2
    n_own = half // CH
    return pl.pallas_call(
        functools.partial(sum_kernel, n_own),
        out_shape=jax.ShapeDtypeStruct(x.shape, jnp.float32),
        in_specs=[pl.BlockSpec(memory_space=pltpu.VMEM)],
        out_specs=pl.BlockSpec(memory_space=pltpu.VMEM),
        scratch_shapes=[pltpu.VMEM((half, 128), jnp.float32), pltpu.VMEM((half, 128), jnp.float32),
                        pltpu.VMEM(((CHIPS - 1) * CH, 128), jnp.float32), pltpu.VMEM((CH, 128), jnp.float32),
                        pltpu.SemaphoreType.DMA((8,))],
        compiler_params=pltpu.CompilerParams(collective_id=cid, has_side_effects=True),
        name="sum_rows",
    )(x)


def gram_of(left_mat, right_mat):
    return lax.dot_general(left_mat, right_mat, (((0,), (0,)), ((), ())), precision=HIGHEST, preferred_element_type=jnp.float32)


TILES = [(i, j) for i in range(4) for j in range(i + 1)]


def pack(gram):
    return jnp.concatenate([gram[i * 128:(i + 1) * 128, j * 128:(j + 1) * 128] for i, j in TILES], axis=0)


def unpack(tiles):
    blk = {ij: tiles[k * 128:(k + 1) * 128] for k, ij in enumerate(TILES)}
    return jnp.concatenate([jnp.concatenate([blk[i, j] if i >= j else blk[j, i].T for j in range(4)], axis=1) for i in range(4)], axis=0)


def solution(mesh):
    def group_solve(a_blk, b_blk):
        gram_one = unpack(sum_all(pack(gram_of(a_blk, a_blk)), 0))
        low_one = jnp.linalg.cholesky(gram_one)
        q_one = lax.linalg.triangular_solve(low_one, a_blk, left_side=False, lower=True, transpose_a=True)
        both = sum_all(jnp.concatenate([pack(gram_of(q_one, q_one)), gram_of(q_one, b_blk)], axis=0), 1)
        gram_two, proj_one = unpack(both[:1280]), both[1280:]
        low_two = jnp.linalg.cholesky(gram_two)
        proj_two = lax.linalg.triangular_solve(low_two, proj_one, left_side=True, lower=True)
        low_prod = jnp.dot(low_one, low_two, precision=HIGHEST, preferred_element_type=jnp.float32)
        x_sol = lax.linalg.triangular_solve(low_prod, proj_two, left_side=True, lower=True, transpose_a=True)
        return x_sol, low_prod.T

    row_spec = P(("batch", "rows"), None)
    out_spec = P("batch", None)
    return jax.shard_map(group_solve, mesh=mesh, in_specs=(row_spec, row_spec), out_specs=(out_spec, out_spec), check_vma=False)
```

```python
import functools
import jax, jax.numpy as jnp
from jax import lax
from jax.experimental import pallas as pl
from jax.experimental.pallas import tpu as pltpu
from jax.sharding import PartitionSpec as P

HIGHEST = lax.Precision.HIGHEST
CHIPS = 64
CH = 16


def owner_index(chip, n_own):
    idx = (chip * n_own + CHIPS - 1) // CHIPS
    return idx, jnp.logical_and((idx * CHIPS) // n_own == chip, idx < n_own)


def sum_kernel(n_own, x_ref, o_ref, pair_buf, part, rs_buf, red, sems):
    dev = lax.axis_index("rows")
    chip, core = dev // 2, dev % 2
    half = n_own * CH
    mine = pl.multiple_of(core * half, CH)
    other = pl.multiple_of((1 - core) * half, CH)
    partner = {"rows": chip * 2 + 1 - core}

    def peer(step):
        t = (chip + step) % CHIPS
        return t, {"rows": t * 2 + core}

    barrier = pltpu.get_barrier_semaphore()
    pl.semaphore_signal(barrier, inc=1, device_id=partner)

    @pl.loop(1, CHIPS)
    def _(step):
        pl.semaphore_signal(barrier, inc=1, device_id=peer(step)[1])
    pl.semaphore_wait(barrier, CHIPS)

    pair = pltpu.make_async_remote_copy(x_ref.at[pl.ds(other, half)], pair_buf, sems.at[0], sems.at[1], device_id=partner)
    pair.start()
    pair.wait()
    part[...] = x_ref[pl.ds(mine, half), :] + pair_buf[...]

    my_idx, owner = owner_index(chip, n_own)
    my_row = pl.multiple_of(my_idx * CH, CH)

    @pl.loop(1, CHIPS)
    def _(step):
        t, dst = peer(step)
        idx, owns = owner_index(t, n_own)

        @pl.when(owns)
        def _():
            pltpu.make_async_remote_copy(part.at[pl.ds(pl.multiple_of(idx * CH, CH), CH)],
                                         rs_buf.at[pl.ds(pl.multiple_of((step - 1) * CH, CH), CH)],
                                         sems.at[2], sems.at[3], device_id=dst).start()

    def wait_rows(n, sem):
        pltpu.make_async_copy(part.at[pl.ds(0, n * CH)], part.at[pl.ds(0, n * CH)], sem).wait()

    @pl.when(owner)
    def _():
        pltpu.make_async_copy(rs_buf, rs_buf, sems.at[3]).wait()
        tot = part[pl.ds(my_row, CH), :]
        for s in range(CHIPS - 1):
            tot = tot + rs_buf[pl.ds(s * CH, CH), :]
        red[...] = tot
        o_ref[pl.ds(mine + my_row, CH), :] = tot

        @pl.loop(1, CHIPS)
        def _(step):
            pltpu.make_async_remote_copy(red, o_ref.at[pl.ds(pl.multiple_of(mine + my_row, CH), CH)],
                                         sems.at[4], sems.at[5], device_id=peer(step)[1]).start()
        wait_rows(n_own - 1, sems.at[2])
        wait_rows(n_own - 1, sems.at[5])

    @pl.when(jnp.logical_not(owner))
    def _():
        wait_rows(n_own, sems.at[2])
        wait_rows(n_own, sems.at[5])

    swap = pltpu.make_async_remote_copy(o_ref.at[pl.ds(mine, half)], o_ref.at[pl.ds(mine, half)], sems.at[6], sems.at[7], device_id=partner)
    swap.start()
    swap.wait()

    @pl.when(owner)
    def _():
        pltpu.make_async_copy(rs_buf, rs_buf, sems.at[4]).wait()


def sum_all(x, cid):
    rows = x.shape[0]
    half = rows // 2
    n_own = half // CH
    return pl.pallas_call(
        functools.partial(sum_kernel, n_own),
        out_shape=jax.ShapeDtypeStruct(x.shape, jnp.float32),
        in_specs=[pl.BlockSpec(memory_space=pltpu.VMEM)],
        out_specs=pl.BlockSpec(memory_space=pltpu.VMEM),
        scratch_shapes=[pltpu.VMEM((half, 128), jnp.float32), pltpu.VMEM((half, 128), jnp.float32),
                        pltpu.VMEM(((CHIPS - 1) * CH, 128), jnp.float32), pltpu.VMEM((CH, 128), jnp.float32),
                        pltpu.SemaphoreType.DMA((8,))],
        compiler_params=pltpu.CompilerParams(collective_id=cid, has_side_effects=True),
        name="sum_rows",
    )(x)


TRI = [(j, i) for j in range(4) for i in range(j, 4)]
TILE = 512
GIVE = 60 * 1024 * 1024


def mm(a, b):
    return lax.dot_general(a, b, (((1,), (0,)), ((), ())), precision=HIGHEST, preferred_element_type=jnp.float32)


def mm_t(a, b):
    return lax.dot_general(a, b, (((0,), (0,)), ((), ())), precision=HIGHEST, preferred_element_type=jnp.float32)


def pack_into(o_ref, g_ref):
    for t, (j, i) in enumerate(TRI):
        o_ref[t * 128:t * 128 + 128, :] = g_ref[j * 128:j * 128 + 128, i * 128:i * 128 + 128]


def gram_kernel(a_ref, o_ref, acc):
    step = pl.program_id(0)

    @pl.when(step == 0)
    def _():
        acc[...] = jnp.zeros_like(acc)
    acc[:256, :] += mm_t(a_ref[:, :256], a_ref[...])
    acc[256:, 256:] += mm_t(a_ref[:, 256:], a_ref[:, 256:])

    @pl.when(step == pl.num_programs(0) - 1)
    def _():
        pack_into(o_ref, acc)


def local_gram(a_blk):
    rows = a_blk.shape[0]
    return pl.pallas_call(
        gram_kernel, grid=(rows // TILE,),
        out_shape=jax.ShapeDtypeStruct((1280, 128), jnp.float32),
        in_specs=[pl.BlockSpec((TILE, 512), lambda i: (i, 0))],
        out_specs=pl.BlockSpec((1280, 128), lambda i: (0, 0)),
        scratch_shapes=[pltpu.VMEM((512, 512), jnp.float32)],
        compiler_params=pltpu.CompilerParams(dimension_semantics=("arbitrary",), vmem_limit_bytes=GIVE),
        name="gram_one",
    )(a_blk)


def second_kernel(a_ref, b_ref, r_ref, x_ref, o_ref, acc, proj):
    step = pl.program_id(0)

    @pl.when(step == 0)
    def _():
        acc[...] = jnp.zeros_like(acc)
        proj[...] = jnp.zeros_like(proj)
    q_lo = mm(a_ref[:, :256], x_ref[:256, :])
    q_hi = mm(a_ref[:, 256:] - mm(q_lo, r_ref[:256, 256:]), x_ref[256:, :])
    b_blk = b_ref[...]
    acc[:256, :256] += mm_t(q_lo, q_lo)
    acc[:256, 256:] += mm_t(q_lo, q_hi)
    acc[256:, 256:] += mm_t(q_hi, q_hi)
    proj[:256, :] += mm_t(q_lo, b_blk)
    proj[256:, :] += mm_t(q_hi, b_blk)

    @pl.when(step == pl.num_programs(0) - 1)
    def _():
        pack_into(o_ref, acc)
        o_ref[1280:, :] = proj[...]


def second_pass(a_blk, b_blk, r_one, x_one):
    rows = a_blk.shape[0]
    return pl.pallas_call(
        second_kernel, grid=(rows // TILE,),
        out_shape=jax.ShapeDtypeStruct((1792, 128), jnp.float32),
        in_specs=[pl.BlockSpec((TILE, 512), lambda i: (i, 0)), pl.BlockSpec((TILE, 128), lambda i: (i, 0)),
                  pl.BlockSpec((512, 512), lambda i: (0, 0)), pl.BlockSpec((512, 256), lambda i: (0, 0))],
        out_specs=pl.BlockSpec((1792, 128), lambda i: (0, 0)),
        scratch_shapes=[pltpu.VMEM((512, 512), jnp.float32), pltpu.VMEM((512, 128), jnp.float32)],
        compiler_params=pltpu.CompilerParams(dimension_semantics=("arbitrary",), vmem_limit_bytes=GIVE),
        name="second_pass",
    )(a_blk, b_blk, r_one, x_one)


def factor_block(d_mat):
    sub = lax.broadcasted_iota(jnp.int32, (8, 128), 0)
    lane = lax.broadcasted_iota(jnp.int32, (8, 128), 1)
    d_row = lax.broadcasted_iota(jnp.int32, (128, 128), 0)
    d_col = lax.broadcasted_iota(jnp.int32, (128, 128), 1)
    d_mat = jnp.where(d_col >= d_row, d_mat, d_mat.T)
    rows = [d_mat[8 * i:8 * i + 8, :] for i in range(16)]
    inv = [jnp.where(lane == sub + 8 * i, 1.0, 0.0).astype(jnp.float32) for i in range(16)]
    r_out, v_out = [], []
    for k in range(16):
        cols = {i: [jnp.broadcast_to(rows[i][:, 8 * k + r:8 * k + r + 1], (8, 128)) for r in range(8)] for i in range(k, 16)}
        scale = jnp.zeros((8, 128), jnp.float32)
        top = cols[k]
        for r in range(8):
            inv_root = lax.rsqrt(jnp.broadcast_to(top[r][r:r + 1, :], (8, 128)))
            scale = jnp.where(sub == r, inv_root, scale)
            below = jnp.where(sub > r, top[r] * inv_root, 0.0)
            row_s = jnp.broadcast_to(rows[k][r:r + 1, :], (8, 128)) * inv_root
            row_v = jnp.broadcast_to(inv[k][r:r + 1, :], (8, 128)) * inv_root
            coef = [jnp.broadcast_to(top[c][r:r + 1, :], (8, 128)) * inv_root for c in range(r + 1, 8)]
            for c in range(r + 1, 8):
                top[c] = top[c] - below * coef[c - r - 1]
            rows[k] = rows[k] - below * row_s
            inv[k] = inv[k] - below * row_v
            for i in range(k + 1, 16):
                mult = cols[i][r] * inv_root
                for c in range(r + 1, 8):
                    cols[i][c] = cols[i][c] - mult * coef[c - r - 1]
                rows[i] = rows[i] - mult * row_s
                inv[i] = inv[i] - mult * row_v
        r_out.append(jnp.where(lane >= sub + 8 * k, rows[k] * scale, 0.0))
        v_out.append(inv[k] * scale)
    return r_out, v_out


def factor(g_ref, r_out, x_out, s_mat, v_mat, r_mat):
    width = s_mat.shape[1]
    for t, (j, i) in enumerate(TRI):
        s_mat[j * 128:j * 128 + 128, i * 128:i * 128 + 128] = g_ref[t * 128:t * 128 + 128, :]
    if width > 512:
        s_mat[:, 512:] = g_ref[1280:, :]

    @pl.loop(0, 4)
    def _(j):
        top = pl.multiple_of(j * 128, 128)
        r_blk, v_blk = factor_block(s_mat[pl.ds(top, 128), pl.ds(top, 128)])
        for i in range(16):
            r_mat[pl.ds(top + 8 * i, 8), pl.ds(top, 128)] = r_blk[i]
            v_mat[pl.ds(top + 8 * i, 8), :] = v_blk[i]
        for jj in range(4):
            lo, hi = 128 * jj, 128 * jj + 128
            if hi < width:
                @pl.when(j == jj)
                def _():
                    row = mm(v_mat[lo:hi, :], s_mat[lo:hi, hi:])
                    r_mat[lo:hi, hi:] = row
                    if hi < 512:
                        s_mat[hi:, hi:] = s_mat[hi:, hi:] - mm_t(row[:, :512 - hi], row)
    for jj in range(1, 4):
        r_mat[128 * jj:128 * jj + 128, :128 * jj] = jnp.zeros((128, 128 * jj), jnp.float32)
    for p in range(2):
        lo, mid, hi = 256 * p, 256 * p + 128, 256 * p + 256
        x_lo, x_hi = v_mat[lo:mid, :].T, v_mat[mid:hi, :].T
        x_out[lo:mid, :128] = x_lo
        x_out[mid:hi, 128:] = x_hi
        x_out[mid:hi, :128] = jnp.zeros((128, 128), jnp.float32)
        x_out[lo:mid, 128:] = -mm(x_lo, mm(r_mat[lo:mid, mid:hi], x_hi))


def chol_kernel(g_ref, r_out, x_out, s_mat, v_mat):
    factor(g_ref, r_out, x_out, s_mat, v_mat, r_out)


def chol_one(tiles):
    return pl.pallas_call(
        chol_kernel,
        out_shape=(jax.ShapeDtypeStruct((512, 512), jnp.float32), jax.ShapeDtypeStruct((512, 256), jnp.float32)),
        in_specs=[pl.BlockSpec(memory_space=pltpu.VMEM)],
        out_specs=(pl.BlockSpec(memory_space=pltpu.VMEM),) * 2,
        scratch_shapes=[pltpu.VMEM((512, 512), jnp.float32), pltpu.VMEM((512, 128), jnp.float32)],
        compiler_params=pltpu.CompilerParams(vmem_limit_bytes=GIVE),
        name="chol_one",
    )(tiles)


def back_solve(r_ref, x_ref, y_lo, y_hi):
    z_hi = mm(x_ref[256:, :], y_hi)
    z_lo = mm(x_ref[:256, :], y_lo - mm(r_ref[:256, 256:512], z_hi))
    return z_lo, z_hi


def last_kernel(g_ref, r_one, x_one, sol, r_fac, s_mat, v_mat, r_two, x_two):
    factor(g_ref, r_two, x_two, s_mat, v_mat, r_two)
    z_lo, z_hi = back_solve(r_two, x_two, r_two[:256, 512:], r_two[256:, 512:])
    s_lo, s_hi = back_solve(r_one, x_one, z_lo, z_hi)
    sol[:256, :] = s_lo
    sol[256:, :] = s_hi
    r_fac[:256, :256] = mm(r_two[:256, :256], r_one[:256, :256])
    r_fac[:256, 256:] = mm(r_two[:256, :512], r_one[:, 256:])
    r_fac[256:, 256:] = mm(r_two[256:, 256:512], r_one[256:, 256:])
    r_fac[256:, :256] = jnp.zeros((256, 256), jnp.float32)


def finish(tiles, r_one, x_one):
    return pl.pallas_call(
        last_kernel,
        out_shape=(jax.ShapeDtypeStruct((512, 128), jnp.float32), jax.ShapeDtypeStruct((512, 512), jnp.float32)),
        in_specs=[pl.BlockSpec(memory_space=pltpu.VMEM)] * 3,
        out_specs=(pl.BlockSpec(memory_space=pltpu.VMEM),) * 2,
        scratch_shapes=[pltpu.VMEM((512, 640), jnp.float32), pltpu.VMEM((512, 128), jnp.float32),
                        pltpu.VMEM((512, 640), jnp.float32), pltpu.VMEM((512, 256), jnp.float32)],
        compiler_params=pltpu.CompilerParams(vmem_limit_bytes=GIVE),
        name="finish",
    )(tiles, r_one, x_one)


def solution(mesh):
    def group_solve(a_blk, b_blk):
        r_one, x_one = chol_one(sum_all(local_gram(a_blk), 0))
        return finish(sum_all(second_pass(a_blk, b_blk, r_one, x_one), 1), r_one, x_one)

    row_spec = P(("batch", "rows"), None)
    out_spec = P("batch", None)
    return jax.shard_map(group_solve, mesh=mesh, in_specs=(row_spec, row_spec), out_specs=(out_spec, out_spec), check_vma=False)
```

```python
import jax
import jax.numpy as jnp
from jax import lax
from jax.experimental import pallas as pl
from jax.experimental.pallas import tpu as pltpu
from jax.sharding import PartitionSpec as P

HIGHEST = lax.Precision.HIGHEST
CHIPS = 64
CH = 16
TRI = [(j, i) for j in range(4) for i in range(j, 4)]
TILE = 512
GIVE = 60 * 1024 * 1024


def mm(a, b):
    return lax.dot_general(a, b, (((1,), (0,)), ((), ())), precision=HIGHEST, preferred_element_type=jnp.float32)


def mm_t(a, b):
    return lax.dot_general(a, b, (((0,), (0,)), ((), ())), precision=HIGHEST, preferred_element_type=jnp.float32)


def pack_into(o_ref, g_ref):
    for t, (j, i) in enumerate(TRI):
        o_ref[t * 128:t * 128 + 128, :] = g_ref[j * 128:j * 128 + 128, i * 128:i * 128 + 128]


def owner_index(chip, n_own):
    idx = (chip * n_own + CHIPS - 1) // CHIPS
    return idx, jnp.logical_and((idx * CHIPS) // n_own == chip, idx < n_own)


def place():
    dev = lax.axis_index("rows")
    return dev // 2, dev % 2


def peer(chip, core, step):
    t = (chip + step) % CHIPS
    return t, {"rows": t * 2 + core}


def greet(barrier):
    chip, core = place()
    pl.semaphore_signal(barrier, inc=1, device_id={"rows": chip * 2 + 1 - core})

    @pl.loop(1, CHIPS)
    def _(step):
        pl.semaphore_signal(barrier, inc=1, device_id=peer(chip, core, step)[1])


def sum_all(x_ref, o_ref, pair_buf, part, rs_buf, red, sems):
    chip, core = place()
    half = x_ref.shape[0] // 2
    n_own = half // CH
    mine = pl.multiple_of(core * half, CH)
    other = pl.multiple_of((1 - core) * half, CH)
    partner = {"rows": chip * 2 + 1 - core}

    pair = pltpu.make_async_remote_copy(x_ref.at[pl.ds(other, half)], pair_buf, sems.at[0], sems.at[1], device_id=partner)
    pair.start()
    pair.wait()
    part[...] = x_ref[pl.ds(mine, half), :] + pair_buf[...]

    my_idx, owner = owner_index(chip, n_own)
    my_row = pl.multiple_of(my_idx * CH, CH)

    @pl.loop(1, CHIPS)
    def _(step):
        t, dst = peer(chip, core, step)
        idx, owns = owner_index(t, n_own)

        @pl.when(owns)
        def _():
            pltpu.make_async_remote_copy(part.at[pl.ds(pl.multiple_of(idx * CH, CH), CH)],
                                         rs_buf.at[pl.ds(pl.multiple_of((step - 1) * CH, CH), CH)],
                                         sems.at[2], sems.at[3], device_id=dst).start()

    def wait_rows(n, sem):
        pltpu.make_async_copy(part.at[pl.ds(0, n * CH)], part.at[pl.ds(0, n * CH)], sem).wait()

    @pl.when(owner)
    def _():
        pltpu.make_async_copy(rs_buf, rs_buf, sems.at[3]).wait()
        tot = part[pl.ds(my_row, CH), :]
        for s in range(CHIPS - 1):
            tot = tot + rs_buf[pl.ds(s * CH, CH), :]
        red[...] = tot
        o_ref[pl.ds(mine + my_row, CH), :] = tot

        @pl.loop(1, CHIPS)
        def _(step):
            pltpu.make_async_remote_copy(red, o_ref.at[pl.ds(pl.multiple_of(mine + my_row, CH), CH)],
                                         sems.at[4], sems.at[5], device_id=peer(chip, core, step)[1]).start()
        wait_rows(n_own - 1, sems.at[2])
        wait_rows(n_own - 1, sems.at[5])

    @pl.when(jnp.logical_not(owner))
    def _():
        wait_rows(n_own, sems.at[2])
        wait_rows(n_own, sems.at[5])

    swap = pltpu.make_async_remote_copy(o_ref.at[pl.ds(mine, half)], o_ref.at[pl.ds(mine, half)], sems.at[6], sems.at[7], device_id=partner)
    swap.start()
    swap.wait()

    @pl.when(owner)
    def _():
        pltpu.make_async_copy(rs_buf, rs_buf, sems.at[4]).wait()


def factor_block(d_mat):
    sub = lax.broadcasted_iota(jnp.int32, (8, 128), 0)
    lane = lax.broadcasted_iota(jnp.int32, (8, 128), 1)
    d_row = lax.broadcasted_iota(jnp.int32, (128, 128), 0)
    d_col = lax.broadcasted_iota(jnp.int32, (128, 128), 1)
    d_mat = jnp.where(d_col >= d_row, d_mat, d_mat.T)
    rows = [d_mat[8 * i:8 * i + 8, :] for i in range(16)]
    inv = [jnp.where(lane == sub + 8 * i, 1.0, 0.0).astype(jnp.float32) for i in range(16)]
    r_out, v_out = [], []
    for k in range(16):
        cols = {i: [jnp.broadcast_to(rows[i][:, 8 * k + r:8 * k + r + 1], (8, 128)) for r in range(8)] for i in range(k, 16)}
        scale = jnp.zeros((8, 128), jnp.float32)
        top = cols[k]
        for r in range(8):
            inv_root = lax.rsqrt(jnp.broadcast_to(top[r][r:r + 1, :], (8, 128)))
            scale = jnp.where(sub == r, inv_root, scale)
            below = jnp.where(sub > r, top[r] * inv_root, 0.0)
            row_s = jnp.broadcast_to(rows[k][r:r + 1, :], (8, 128)) * inv_root
            row_v = jnp.broadcast_to(inv[k][r:r + 1, :], (8, 128)) * inv_root
            coef = [jnp.broadcast_to(top[c][r:r + 1, :], (8, 128)) * inv_root for c in range(r + 1, 8)]
            for c in range(r + 1, 8):
                top[c] = top[c] - below * coef[c - r - 1]
            rows[k] = rows[k] - below * row_s
            inv[k] = inv[k] - below * row_v
            for i in range(k + 1, 16):
                mult = cols[i][r] * inv_root
                for c in range(r + 1, 8):
                    cols[i][c] = cols[i][c] - mult * coef[c - r - 1]
                rows[i] = rows[i] - mult * row_s
                inv[i] = inv[i] - mult * row_v
        r_out.append(jnp.where(lane >= sub + 8 * k, rows[k] * scale, 0.0))
        v_out.append(inv[k] * scale)
    return r_out, v_out


def factor(g_ref, r_out, x_out, s_mat, v_mat, r_mat):
    width = s_mat.shape[1]
    for t, (j, i) in enumerate(TRI):
        s_mat[j * 128:j * 128 + 128, i * 128:i * 128 + 128] = g_ref[t * 128:t * 128 + 128, :]
    if width > 512:
        s_mat[:, 512:] = g_ref[1280:, :]

    @pl.loop(0, 4)
    def _(j):
        top = pl.multiple_of(j * 128, 128)
        r_blk, v_blk = factor_block(s_mat[pl.ds(top, 128), pl.ds(top, 128)])
        for i in range(16):
            r_mat[pl.ds(top + 8 * i, 8), pl.ds(top, 128)] = r_blk[i]
            v_mat[pl.ds(top + 8 * i, 8), :] = v_blk[i]
        for jj in range(4):
            lo, hi = 128 * jj, 128 * jj + 128
            if hi < width:
                @pl.when(j == jj)
                def _():
                    row = mm(v_mat[lo:hi, :], s_mat[lo:hi, hi:])
                    r_mat[lo:hi, hi:] = row
                    if hi < 512:
                        s_mat[hi:, hi:] = s_mat[hi:, hi:] - mm_t(row[:, :512 - hi], row)
    for jj in range(1, 4):
        r_mat[128 * jj:128 * jj + 128, :128 * jj] = jnp.zeros((128, 128 * jj), jnp.float32)
    for p in range(2):
        lo, mid, hi = 256 * p, 256 * p + 128, 256 * p + 256
        x_lo, x_hi = v_mat[lo:mid, :].T, v_mat[mid:hi, :].T
        x_out[lo:mid, :128] = x_lo
        x_out[mid:hi, 128:] = x_hi
        x_out[mid:hi, :128] = jnp.zeros((128, 128), jnp.float32)
        x_out[lo:mid, 128:] = -mm(x_lo, mm(r_mat[lo:mid, mid:hi], x_hi))


def back_solve(r_ref, x_ref, y_lo, y_hi):
    z_hi = mm(x_ref[256:, :], y_hi)
    z_lo = mm(x_ref[:256, :], y_lo - mm(r_ref[:256, 256:512], z_hi))
    return z_lo, z_hi


def solve_kernel(a_hbm, b_hbm, sol, r_fac, a_buf, b_buf, acc, proj, x_g, o_g, x_h, o_h, pair_g, part_g, rs_g, red_g,
                 pair_h, part_h, rs_h, red_h, s_one, v_one, r_one, x_one, s_two, v_two, r_two, x_two, load_sem, sems_g, sems_h):
    rows = a_hbm.shape[0]
    steps = rows // TILE

    def tile(i):
        return pl.ds(pl.multiple_of(i * TILE, TILE), TILE)

    def load_a(i):
        return pltpu.make_async_copy(a_hbm.at[tile(i)], a_buf.at[tile(i)], load_sem.at[i])

    load_b = pltpu.make_async_copy(b_hbm, b_buf, load_sem.at[steps])
    for i in range(steps):
        load_a(i).start()
    load_b.start()
    barrier = pltpu.get_barrier_semaphore()
    greet(barrier)

    acc[...] = jnp.zeros_like(acc)

    @pl.loop(0, steps)
    def _(i):
        load_a(i).wait()
        a_lo, a_hi = a_buf[tile(i), :256], a_buf[tile(i), 256:]
        acc[:256, :] += mm_t(a_lo, a_buf[tile(i), :])
        acc[256:, 256:] += mm_t(a_hi, a_hi)
    pack_into(x_g, acc)
    pl.semaphore_wait(barrier, CHIPS)
    sum_all(x_g, o_g, pair_g, part_g, rs_g, red_g, sems_g)
    factor(o_g, r_one, x_one, s_one, v_one, r_one)

    acc[...] = jnp.zeros_like(acc)
    proj[...] = jnp.zeros_like(proj)
    load_b.wait()

    @pl.loop(0, steps)
    def _(i):
        q_lo = mm(a_buf[tile(i), :256], x_one[:256, :])
        q_hi = mm(a_buf[tile(i), 256:] - mm(q_lo, r_one[:256, 256:]), x_one[256:, :])
        b_blk = b_buf[tile(i), :]
        acc[:256, :256] += mm_t(q_lo, q_lo)
        acc[:256, 256:] += mm_t(q_lo, q_hi)
        acc[256:, 256:] += mm_t(q_hi, q_hi)
        proj[:256, :] += mm_t(q_lo, b_blk)
        proj[256:, :] += mm_t(q_hi, b_blk)
    pack_into(x_h, acc)
    x_h[1280:, :] = proj[...]
    sum_all(x_h, o_h, pair_h, part_h, rs_h, red_h, sems_h)
    factor(o_h, r_two, x_two, s_two, v_two, r_two)

    z_lo, z_hi = back_solve(r_two, x_two, r_two[:256, 512:], r_two[256:, 512:])
    s_lo, s_hi = back_solve(r_one, x_one, z_lo, z_hi)
    sol[:256, :] = s_lo
    sol[256:, :] = s_hi
    r_fac[:256, :256] = mm(r_two[:256, :256], r_one[:256, :256])
    r_fac[:256, 256:] = mm(r_two[:256, :512], r_one[:, 256:])
    r_fac[256:, 256:] = mm(r_two[256:, 256:512], r_one[256:, 256:])
    r_fac[256:, :256] = jnp.zeros((256, 256), jnp.float32)


def solution(mesh):
    def group_solve(a_blk, b_blk):
        rows = a_blk.shape[0]

        def buf(r, c=128):
            return pltpu.VMEM((r, c), jnp.float32)

        def sums(r):
            return [buf(r // 2), buf(r // 2), buf((CHIPS - 1) * CH), buf(CH)]
        return pl.pallas_call(
            solve_kernel,
            out_shape=(jax.ShapeDtypeStruct((512, 128), jnp.float32), jax.ShapeDtypeStruct((512, 512), jnp.float32)),
            in_specs=[pl.BlockSpec(memory_space=pl.ANY)] * 2,
            out_specs=(pl.BlockSpec(memory_space=pltpu.VMEM),) * 2,
            scratch_shapes=[buf(rows, 512), buf(rows), buf(512, 512), buf(512), buf(1280), buf(1280), buf(1792), buf(1792),
                            *sums(1280), *sums(1792),
                            buf(512, 512), buf(512), buf(512, 512), buf(512, 256),
                            buf(512, 640), buf(512), buf(512, 640), buf(512, 256),
                            pltpu.SemaphoreType.DMA((rows // TILE + 1,)), pltpu.SemaphoreType.DMA((8,)), pltpu.SemaphoreType.DMA((8,))],
            compiler_params=pltpu.CompilerParams(collective_id=0, has_side_effects=True, vmem_limit_bytes=GIVE),
            name="solve",
        )(a_blk, b_blk)

    row_spec = P(("batch", "rows"), None)
    out_spec = P("batch", None)
    return jax.shard_map(group_solve, mesh=mesh, in_specs=(row_spec, row_spec), out_specs=(out_spec, out_spec), check_vma=False)
```

```python
import jax
import jax.numpy as jnp
from jax import lax
from jax.experimental import pallas as pl
from jax.experimental.pallas import tpu as pltpu
from jax.sharding import PartitionSpec as P

HIGHEST = lax.Precision.HIGHEST
CHIPS = 64
CH = 8
SPREAD, UNSPREAD = 27, 19
LOAD = 512
TILE = 1024
GIVE = 60 * 1024 * 1024
LOLO = [(0, 0), (0, 1), (1, 1)]
LOHI = [(0, 2), (0, 3), (1, 2), (1, 3)]
HIHI = [(2, 2), (2, 3), (3, 3)]


def mm(a, b):
    return lax.dot_general(a, b, (((1,), (0,)), ((), ())), precision=HIGHEST, preferred_element_type=jnp.float32)


def mm_t(a, b):
    return lax.dot_general(a, b, (((0,), (0,)), ((), ())), precision=HIGHEST, preferred_element_type=jnp.float32)


def block(ref, j, i):
    return ref.at[j * 128:j * 128 + 128, i * 128:i * 128 + 128]


def place():
    dev = lax.axis_index("rows")
    return dev // 2, dev % 2


def greet(barrier):
    chip, core = place()
    pl.semaphore_signal(barrier, inc=1, device_id={"rows": chip * 2 + 1 - core})

    @pl.loop(1, CHIPS)
    def _(step):
        pl.semaphore_signal(barrier, inc=1, device_id={"rows": ((chip + step) % CHIPS) * 2 + core})


class Piece:
    def __init__(self, refs, offset):
        self.x, self.o, self.pair_buf, self.part, self.rs_buf, self.red, self.sems = refs
        self.offset = offset
        self.half = self.x.shape[0] // 2
        self.n_own = self.half // CH
        self.chip, self.core = place()
        self.mine = pl.multiple_of(self.core * self.half, CH)
        self.other = pl.multiple_of((1 - self.core) * self.half, CH)
        self.partner = {"rows": self.chip * 2 + 1 - self.core}
        self.idx = (self.chip * UNSPREAD + CHIPS - offset % CHIPS) % CHIPS
        self.owner = self.idx < self.n_own
        self.row = pl.multiple_of(self.idx * CH, CH)

    def swap_in(self):
        return pltpu.make_async_remote_copy(self.x.at[pl.ds(self.other, self.half)], self.pair_buf,
                                            self.sems.at[0], self.sems.at[1], device_id=self.partner)

    def swap_out(self):
        here = self.o.at[pl.ds(self.mine, self.half)]
        return pltpu.make_async_remote_copy(here, here, self.sems.at[6], self.sems.at[7], device_id=self.partner)

    def rows_of(self, n):
        return self.part.at[pl.ds(0, n * CH)]

    def start(self):
        self.swap_in().start()

    def scatter(self):
        self.swap_in().wait()
        self.part[...] = self.x[pl.ds(self.mine, self.half), :] + self.pair_buf[...]

        @pl.loop(0, self.n_own)
        def _(step):
            j = (step + self.chip) % self.n_own
            t = ((j + self.offset) * SPREAD) % CHIPS
            slot = (self.chip + CHIPS - t) % CHIPS - 1

            @pl.when(t != self.chip)
            def _():
                pltpu.make_async_remote_copy(self.part.at[pl.ds(pl.multiple_of(j * CH, CH), CH)],
                                             self.rs_buf.at[pl.ds(pl.multiple_of(slot * CH, CH), CH)],
                                             self.sems.at[2], self.sems.at[3], device_id={"rows": t * 2 + self.core}).start()

    def gather(self):
        @pl.when(self.owner)
        def _():
            pltpu.make_async_copy(self.rs_buf, self.rs_buf, self.sems.at[3]).wait()
            lanes = [self.part[pl.ds(self.row, CH), :]] + [self.rs_buf[s * CH:s * CH + CH, :] for s in range(CHIPS - 1)]
            while len(lanes) > 1:
                lanes = [u + v for u, v in zip(lanes[::2], lanes[1::2])]
            self.red[...] = lanes[0]
            self.o[pl.ds(self.mine + self.row, CH), :] = lanes[0]
            there = self.o.at[pl.ds(pl.multiple_of(self.mine + self.row, CH), CH)]

            @pl.loop(1, CHIPS)
            def _(step):
                pltpu.make_async_remote_copy(self.red, there, self.sems.at[4], self.sems.at[5],
                                             device_id={"rows": ((self.chip + step) % CHIPS) * 2 + self.core}).start()

    def spread(self):
        for own, n in ((True, self.n_own - 1), (False, self.n_own)):
            @pl.when(self.owner == own)
            def _():
                pltpu.make_async_copy(self.rows_of(n), self.rows_of(n), self.sems.at[5]).wait()
        self.swap_out().start()

    def finish(self):
        self.swap_out().wait()
        for own, n in ((True, self.n_own - 1), (False, self.n_own)):
            @pl.when(self.owner == own)
            def _():
                pltpu.make_async_copy(self.rows_of(n), self.rows_of(n), self.sems.at[2]).wait()

        @pl.when(self.owner)
        def _():
            pltpu.make_async_copy(self.rs_buf, self.rs_buf, self.sems.at[4]).wait()


def pack(ref, blocks):
    for t, blk in enumerate(blocks):
        ref[t * 128:t * 128 + 128, :] = blk[...]


def piece_block(ref, t):
    return ref[t * 128:t * 128 + 128, :]


def factor_block(d_mat):
    sub = lax.broadcasted_iota(jnp.int32, (8, 128), 0)
    lane = lax.broadcasted_iota(jnp.int32, (8, 128), 1)
    d_row = lax.broadcasted_iota(jnp.int32, (128, 128), 0)
    d_col = lax.broadcasted_iota(jnp.int32, (128, 128), 1)
    d_mat = jnp.where(d_col >= d_row, d_mat, d_mat.T)
    rows = [d_mat[8 * i:8 * i + 8, :] for i in range(16)]
    inv = [jnp.where(lane == sub + 8 * i, 1.0, 0.0).astype(jnp.float32) for i in range(16)]
    r_out, v_out = [], []
    for k in range(16):
        cols = {i: [jnp.broadcast_to(rows[i][:, 8 * k + r:8 * k + r + 1], (8, 128)) for r in range(8)] for i in range(k, 16)}
        scale = jnp.zeros((8, 128), jnp.float32)
        top = cols[k]
        for r in range(8):
            inv_root = lax.rsqrt(jnp.broadcast_to(top[r][r:r + 1, :], (8, 128)))
            scale = jnp.where(sub == r, inv_root, scale)
            below = jnp.where(sub > r, top[r] * inv_root, 0.0)
            row_s = jnp.broadcast_to(rows[k][r:r + 1, :], (8, 128)) * inv_root
            row_v = jnp.broadcast_to(inv[k][r:r + 1, :], (8, 128)) * inv_root
            coef = [jnp.broadcast_to(top[c][r:r + 1, :], (8, 128)) * inv_root for c in range(r + 1, 8)]
            for c in range(r + 1, 8):
                top[c] = top[c] - below * coef[c - r - 1]
            rows[k] = rows[k] - below * row_s
            inv[k] = inv[k] - below * row_v
            for i in range(k + 1, 16):
                mult = cols[i][r] * inv_root
                for c in range(r + 1, 8):
                    cols[i][c] = cols[i][c] - mult * coef[c - r - 1]
                rows[i] = rows[i] - mult * row_s
                inv[i] = inv[i] - mult * row_v
        r_out.append(jnp.where(lane >= sub + 8 * k, rows[k] * scale, 0.0))
        v_out.append(inv[k] * scale)
    return r_out, v_out


def factor(pieces, r_mat, x_out, s_mat, v_mat):
    width = s_mat.shape[1]
    p_lo, p_mid, p_hi = pieces
    s_mat[256:, 256:] = jnp.zeros((256, width - 256), jnp.float32)
    p_lo.finish()
    for t, (j, i) in enumerate(LOLO):
        block(s_mat, j, i)[...] = piece_block(p_lo.o, t)
    if width > 512:
        for t in range(2):
            block(s_mat, t, 4)[...] = piece_block(p_lo.o, 3 + t).T

    @pl.loop(0, 4)
    def _(j):
        top = pl.multiple_of(j * 128, 128)

        @pl.when(j == 2)
        def _():
            p_hi.finish()
            for t, (jj, ii) in enumerate(HIHI):
                block(s_mat, jj, ii)[...] += piece_block(p_hi.o, t)
            if width > 512:
                for t in range(2):
                    block(s_mat, 2 + t, 4)[...] += piece_block(p_hi.o, 3 + t).T
        r_blk, v_blk = factor_block(s_mat[pl.ds(top, 128), pl.ds(top, 128)])
        for i in range(16):
            r_mat[pl.ds(top + 8 * i, 8), pl.ds(top, 128)] = r_blk[i]
            v_mat[pl.ds(top + 8 * i, 8), :] = v_blk[i]

        @pl.when(j == 0)
        def _():
            p_mid.spread()
            p_hi.gather()
            p_mid.finish()
            for t, (jj, ii) in enumerate(LOHI):
                block(s_mat, jj, ii)[...] = piece_block(p_mid.o, t)

        @pl.when(j == 1)
        def _():
            p_hi.spread()
        for jj in range(4):
            lo, hi = 128 * jj, 128 * jj + 128
            if hi < width:
                @pl.when(j == jj)
                def _():
                    row = mm(v_mat[lo:hi, :], s_mat[lo:hi, hi:])
                    r_mat[lo:hi, hi:] = row
                    if hi < 512:
                        s_mat[hi:, hi:] = s_mat[hi:, hi:] - mm_t(row[:, :512 - hi], row)
    for jj in range(1, 4):
        r_mat[128 * jj:128 * jj + 128, :128 * jj] = jnp.zeros((128, 128 * jj), jnp.float32)
    for p in range(2):
        lo, mid, hi = 256 * p, 256 * p + 128, 256 * p + 256
        x_lo, x_hi = v_mat[lo:mid, :].T, v_mat[mid:hi, :].T
        x_out[lo:mid, :128] = x_lo
        x_out[mid:hi, 128:] = x_hi
        x_out[mid:hi, :128] = jnp.zeros((128, 128), jnp.float32)
        x_out[lo:mid, 128:] = -mm(x_lo, mm(r_mat[lo:mid, mid:hi], x_hi))


def back_solve(r_ref, x_ref, y_lo, y_hi):
    z_hi = mm(x_ref[256:, :], y_hi)
    z_lo = mm(x_ref[:256, :], y_lo - mm(r_ref[:256, 256:512], z_hi))
    return z_lo, z_hi


def solve_kernel(a_hbm, b_hbm, sol, r_fac, a_buf, b_buf, acc, proj, *refs):
    piece_refs, (s_one, v_one, r_one, x_one, s_two, v_two, r_two, x_two, load_sem) = refs[:42], refs[42:]
    one = [Piece(piece_refs[7 * p:7 * p + 7], off) for p, off in enumerate((0, 24, 56))]
    two = [Piece(piece_refs[7 * p:7 * p + 7], off) for p, off in zip((3, 4, 5), (0, 40, 72))]
    rows = a_hbm.shape[0]
    steps = rows // TILE

    def tile(i, size=TILE):
        return pl.ds(pl.multiple_of(i * size, size), size)

    def load_a(i):
        return pltpu.make_async_copy(a_hbm.at[tile(i, LOAD)], a_buf.at[tile(i, LOAD)], load_sem.at[i])

    load_b = pltpu.make_async_copy(b_hbm, b_buf, load_sem.at[rows // LOAD])
    for i in range(rows // LOAD):
        load_a(i).start()
    load_b.start()
    barrier = pltpu.get_barrier_semaphore()
    greet(barrier)
    acc[...] = jnp.zeros_like(acc)
    proj[...] = jnp.zeros_like(proj)

    @pl.loop(0, steps)
    def _(i):
        for part in range(TILE // LOAD):
            load_a(i * (TILE // LOAD) + part).wait()
        a_lo = a_buf[tile(i), :256]
        acc[:256, :256] += mm_t(a_lo, a_lo)
    pack(one[0].x, [block(acc, *ij) for ij in LOLO])
    pl.semaphore_wait(barrier, CHIPS)
    one[0].start()

    @pl.loop(0, steps)
    def _(i):
        acc[:256, 256:] += mm_t(a_buf[tile(i), :256], a_buf[tile(i), 256:])

        @pl.when(i == 1)
        def _():
            one[0].scatter()
    pack(one[1].x, [block(acc, *ij) for ij in LOHI])
    one[1].start()

    @pl.loop(0, steps)
    def _(i):
        a_hi = a_buf[tile(i), 256:]
        acc[256:, 256:] += mm_t(a_hi, a_hi)

        @pl.when(i == 1)
        def _():
            one[1].scatter()

        @pl.when(i == 2)
        def _():
            one[0].gather()
    pack(one[2].x, [block(acc, *ij) for ij in HIHI])
    one[2].start()
    one[1].gather()
    one[2].scatter()
    one[0].spread()
    factor(one, r_one, x_one, s_one, v_one)

    acc[...] = jnp.zeros_like(acc)
    load_b.wait()

    @pl.loop(0, steps)
    def _(i):
        q_lo = mm(a_buf[tile(i), :256], x_one[:256, :])
        a_buf[tile(i), :256] = q_lo
        acc[:256, :256] += mm_t(q_lo, q_lo)
        proj[:, :256] += mm_t(b_buf[tile(i), :], q_lo)
    pack(two[0].x, [block(acc, *ij) for ij in LOLO] + [block(proj, 0, i) for i in range(2)])
    two[0].start()

    @pl.loop(0, steps)
    def _(i):
        q_lo = a_buf[tile(i), :256]
        q_hi = mm(a_buf[tile(i), 256:] - mm(q_lo, r_one[:256, 256:]), x_one[256:, :])
        a_buf[tile(i), 256:] = q_hi
        acc[:256, 256:] += mm_t(q_lo, q_hi)

        @pl.when(i == 0)
        def _():
            two[0].scatter()

        @pl.when(i == 2)
        def _():
            two[0].gather()
    pack(two[1].x, [block(acc, *ij) for ij in LOHI])
    two[1].start()

    @pl.loop(0, steps)
    def _(i):
        q_hi = a_buf[tile(i), 256:]
        acc[256:, 256:] += mm_t(q_hi, q_hi)
        proj[:, 256:] += mm_t(b_buf[tile(i), :], q_hi)

        @pl.when(i == 0)
        def _():
            two[1].scatter()

        @pl.when(i == 1)
        def _():
            two[0].spread()
    pack(two[2].x, [block(acc, *ij) for ij in HIHI] + [block(proj, 0, i) for i in range(2, 4)])
    two[2].start()
    two[1].gather()
    two[2].scatter()
    factor(two, r_two, x_two, s_two, v_two)

    z_lo, z_hi = back_solve(r_two, x_two, r_two[:256, 512:], r_two[256:, 512:])
    s_lo, s_hi = back_solve(r_one, x_one, z_lo, z_hi)
    sol[:256, :] = s_lo
    sol[256:, :] = s_hi
    r_fac[:256, :256] = mm(r_two[:256, :256], r_one[:256, :256])
    r_fac[:256, 256:] = mm(r_two[:256, :512], r_one[:, 256:])
    r_fac[256:, 256:] = mm(r_two[256:, 256:512], r_one[256:, 256:])
    r_fac[256:, :256] = jnp.zeros((256, 256), jnp.float32)


def solution(mesh):
    def group_solve(a_blk, b_blk):
        rows = a_blk.shape[0]

        def buf(r, c=128):
            return pltpu.VMEM((r, c), jnp.float32)

        def piece(r):
            return [buf(r), buf(r), buf(r // 2), buf(r // 2), buf((CHIPS - 1) * CH), buf(CH), pltpu.SemaphoreType.DMA((8,))]
        return pl.pallas_call(
            solve_kernel,
            out_shape=(jax.ShapeDtypeStruct((512, 128), jnp.float32), jax.ShapeDtypeStruct((512, 512), jnp.float32)),
            in_specs=[pl.BlockSpec(memory_space=pl.ANY)] * 2,
            out_specs=(pl.BlockSpec(memory_space=pltpu.VMEM),) * 2,
            scratch_shapes=[buf(rows, 512), buf(rows), buf(512, 512), buf(128, 512),
                            *piece(384), *piece(512), *piece(384), *piece(640), *piece(512), *piece(640),
                            buf(512, 512), buf(512), buf(512, 512), buf(512, 256),
                            buf(512, 640), buf(512), buf(512, 640), buf(512, 256),
                            pltpu.SemaphoreType.DMA((rows // LOAD + 1,))],
            compiler_params=pltpu.CompilerParams(collective_id=0, has_side_effects=True, vmem_limit_bytes=GIVE),
            name="solve",
        )(a_blk, b_blk)

    row_spec = P(("batch", "rows"), None)
    out_spec = P("batch", None)
    return jax.shard_map(group_solve, mesh=mesh, in_specs=(row_spec, row_spec), out_specs=(out_spec, out_spec), check_vma=False)
```

```python
import jax
import jax.numpy as jnp
from jax import lax
from jax.experimental import pallas as pl
from jax.experimental.pallas import tpu as pltpu
from jax.sharding import PartitionSpec as P

HIGHEST = lax.Precision.HIGHEST
CHIPS = 64
CH = 8
SPREAD, UNSPREAD = 27, 19
LOAD = 512
TILE = 1024
WIDE = 2048
GIVE = 60 * 1024 * 1024
LOLO = [(0, 0), (0, 1), (1, 1)]
LOHI = [(0, 2), (0, 3), (1, 2), (1, 3)]
HIHI = [(2, 2), (2, 3), (3, 3)]


def mm(a, b):
    return lax.dot_general(a, b, (((1,), (0,)), ((), ())), precision=HIGHEST, preferred_element_type=jnp.float32)


def mm_t(a, b):
    return lax.dot_general(a, b, (((0,), (0,)), ((), ())), precision=HIGHEST, preferred_element_type=jnp.float32)


def block(ref, j, i):
    return ref.at[j * 128:j * 128 + 128, i * 128:i * 128 + 128]


def place():
    dev = lax.axis_index("rows")
    return dev // 2, dev % 2


def greet(barrier):
    chip, core = place()
    pl.semaphore_signal(barrier, inc=1, device_id={"rows": chip * 2 + 1 - core})

    @pl.loop(1, CHIPS)
    def _(step):
        pl.semaphore_signal(barrier, inc=1, device_id={"rows": ((chip + step) % CHIPS) * 2 + core})


class Piece:
    def __init__(self, refs, offset):
        self.x, self.o, self.pair_buf, self.part, self.rs_buf, self.red, self.sems = refs
        self.offset = offset
        self.half = self.x.shape[0] // 2
        self.n_own = self.half // CH
        self.chip, self.core = place()
        self.mine = pl.multiple_of(self.core * self.half, CH)
        self.other = pl.multiple_of((1 - self.core) * self.half, CH)
        self.partner = {"rows": self.chip * 2 + 1 - self.core}
        self.idx = (self.chip * UNSPREAD + CHIPS - offset % CHIPS) % CHIPS
        self.owner = self.idx < self.n_own
        self.row = pl.multiple_of(self.idx * CH, CH)

    def swap_in(self):
        return pltpu.make_async_remote_copy(self.x.at[pl.ds(self.other, self.half)], self.pair_buf,
                                            self.sems.at[0], self.sems.at[1], device_id=self.partner)

    def swap_out(self):
        here = self.o.at[pl.ds(self.mine, self.half)]
        return pltpu.make_async_remote_copy(here, here, self.sems.at[6], self.sems.at[7], device_id=self.partner)

    def rows_of(self, n):
        return self.part.at[pl.ds(0, n * CH)]

    def start(self):
        self.swap_in().start()

    def scatter(self):
        self.swap_in().wait()
        self.part[...] = self.x[pl.ds(self.mine, self.half), :] + self.pair_buf[...]

        @pl.loop(0, self.n_own)
        def _(step):
            j = (step + self.chip) % self.n_own
            t = ((j + self.offset) * SPREAD) % CHIPS
            slot = (self.chip + CHIPS - t) % CHIPS - 1

            @pl.when(t != self.chip)
            def _():
                pltpu.make_async_remote_copy(self.part.at[pl.ds(pl.multiple_of(j * CH, CH), CH)],
                                             self.rs_buf.at[pl.ds(pl.multiple_of(slot * CH, CH), CH)],
                                             self.sems.at[2], self.sems.at[3], device_id={"rows": t * 2 + self.core}).start()

    def gather(self):
        @pl.when(self.owner)
        def _():
            pltpu.make_async_copy(self.rs_buf, self.rs_buf, self.sems.at[3]).wait()
            lanes = [self.part[pl.ds(self.row, CH), :]] + [self.rs_buf[s * CH:s * CH + CH, :] for s in range(CHIPS - 1)]
            while len(lanes) > 1:
                lanes = [u + v for u, v in zip(lanes[::2], lanes[1::2])]
            self.red[...] = lanes[0]
            self.o[pl.ds(self.mine + self.row, CH), :] = lanes[0]
            there = self.o.at[pl.ds(pl.multiple_of(self.mine + self.row, CH), CH)]

            @pl.loop(1, CHIPS)
            def _(step):
                pltpu.make_async_remote_copy(self.red, there, self.sems.at[4], self.sems.at[5],
                                             device_id={"rows": ((self.chip + step) % CHIPS) * 2 + self.core}).start()

    def spread(self):
        for own, n in ((True, self.n_own - 1), (False, self.n_own)):
            @pl.when(self.owner == own)
            def _():
                pltpu.make_async_copy(self.rows_of(n), self.rows_of(n), self.sems.at[5]).wait()
        self.swap_out().start()

    def finish(self):
        self.swap_out().wait()
        for own, n in ((True, self.n_own - 1), (False, self.n_own)):
            @pl.when(self.owner == own)
            def _():
                pltpu.make_async_copy(self.rows_of(n), self.rows_of(n), self.sems.at[2]).wait()

        @pl.when(self.owner)
        def _():
            pltpu.make_async_copy(self.rs_buf, self.rs_buf, self.sems.at[4]).wait()


def pack(ref, blocks):
    for t, blk in enumerate(blocks):
        ref[t * 128:t * 128 + 128, :] = blk[...]


def piece_block(ref, t):
    return ref[t * 128:t * 128 + 128, :]


def factor_block(d_mat):
    sub = lax.broadcasted_iota(jnp.int32, (8, 128), 0)
    lane = lax.broadcasted_iota(jnp.int32, (8, 128), 1)
    d_row = lax.broadcasted_iota(jnp.int32, (128, 128), 0)
    d_col = lax.broadcasted_iota(jnp.int32, (128, 128), 1)
    d_mat = jnp.where(d_col >= d_row, d_mat, d_mat.T)
    rows = [d_mat[8 * i:8 * i + 8, :] for i in range(16)]
    inv = [jnp.where(lane == sub + 8 * i, 1.0, 0.0).astype(jnp.float32) for i in range(16)]
    r_out, v_out = [], []
    for k in range(16):
        cols = {i: [jnp.broadcast_to(rows[i][:, 8 * k + r:8 * k + r + 1], (8, 128)) for r in range(8)] for i in range(k, 16)}
        scale = jnp.zeros((8, 128), jnp.float32)
        top = cols[k]
        for r in range(8):
            inv_root = lax.rsqrt(jnp.broadcast_to(top[r][r:r + 1, :], (8, 128)))
            scale = jnp.where(sub == r, inv_root, scale)
            below = jnp.where(sub > r, top[r] * inv_root, 0.0)
            row_s = jnp.broadcast_to(rows[k][r:r + 1, :], (8, 128)) * inv_root
            row_v = jnp.broadcast_to(inv[k][r:r + 1, :], (8, 128)) * inv_root
            coef = [jnp.broadcast_to(top[c][r:r + 1, :], (8, 128)) * inv_root for c in range(r + 1, 8)]
            for c in range(r + 1, 8):
                top[c] = top[c] - below * coef[c - r - 1]
            rows[k] = rows[k] - below * row_s
            inv[k] = inv[k] - below * row_v
            for i in range(k + 1, 16):
                mult = cols[i][r] * inv_root
                for c in range(r + 1, 8):
                    cols[i][c] = cols[i][c] - mult * coef[c - r - 1]
                rows[i] = rows[i] - mult * row_s
                inv[i] = inv[i] - mult * row_v
        r_out.append(jnp.where(lane >= sub + 8 * k, rows[k] * scale, 0.0))
        v_out.append(inv[k] * scale)
    return r_out, v_out


def factor(pieces, r_mat, x_out, s_mat, v_mat):
    width = s_mat.shape[1]
    p_lo, p_mid, p_hi = pieces
    s_mat[256:, 256:] = jnp.zeros((256, width - 256), jnp.float32)
    p_lo.finish()
    for t, (j, i) in enumerate(LOLO):
        block(s_mat, j, i)[...] = piece_block(p_lo.o, t)
    if width > 512:
        for t in range(2):
            block(s_mat, t, 4)[...] = piece_block(p_lo.o, 3 + t).T

    @pl.loop(0, 4)
    def _(j):
        top = pl.multiple_of(j * 128, 128)

        @pl.when(j == 2)
        def _():
            p_hi.finish()
            for t, (jj, ii) in enumerate(HIHI):
                block(s_mat, jj, ii)[...] += piece_block(p_hi.o, t)
            if width > 512:
                for t in range(2):
                    block(s_mat, 2 + t, 4)[...] += piece_block(p_hi.o, 3 + t).T
        r_blk, v_blk = factor_block(s_mat[pl.ds(top, 128), pl.ds(top, 128)])
        for i in range(16):
            r_mat[pl.ds(top + 8 * i, 8), pl.ds(top, 128)] = r_blk[i]
            v_mat[pl.ds(top + 8 * i, 8), :] = v_blk[i]

        @pl.when(j == 0)
        def _():
            p_mid.spread()
            p_hi.gather()
            p_mid.finish()
            for t, (jj, ii) in enumerate(LOHI):
                block(s_mat, jj, ii)[...] = piece_block(p_mid.o, t)

        @pl.when(j == 1)
        def _():
            p_hi.spread()
        for jj in range(4):
            lo, hi = 128 * jj, 128 * jj + 128
            if hi < width:
                @pl.when(j == jj)
                def _():
                    row = mm(v_mat[lo:hi, :], s_mat[lo:hi, hi:])
                    r_mat[lo:hi, hi:] = row
                    if hi < 512:
                        s_mat[hi:, hi:] = s_mat[hi:, hi:] - mm_t(row[:, :512 - hi], row)
    for jj in range(1, 4):
        r_mat[128 * jj:128 * jj + 128, :128 * jj] = jnp.zeros((128, 128 * jj), jnp.float32)
    for p in range(2):
        lo, mid, hi = 256 * p, 256 * p + 128, 256 * p + 256
        x_lo, x_hi = v_mat[lo:mid, :].T, v_mat[mid:hi, :].T
        x_out[lo:mid, lo:mid] = x_lo
        x_out[mid:hi, mid:hi] = x_hi
        x_out[mid:hi, lo:mid] = jnp.zeros((128, 128), jnp.float32)
        x_out[lo:mid, mid:hi] = -mm(x_lo, mm(r_mat[lo:mid, mid:hi], x_hi))
    x_out[256:, :256] = jnp.zeros((256, 256), jnp.float32)
    x_out[:256, 256:] = -mm(mm(x_out[:256, :256], r_mat[:256, 256:512]), x_out[256:, 256:])


def solve_kernel(a_hbm, b_hbm, sol, r_fac, a_buf, q_lo, b_buf, acc, proj, *refs):
    piece_refs, (s_one, v_one, r_one, x_one, s_two, v_two, r_two, x_two, load_sem) = refs[:42], refs[42:]
    one = [Piece(piece_refs[7 * p:7 * p + 7], off) for p, off in enumerate((0, 24, 56))]
    two = [Piece(piece_refs[7 * p:7 * p + 7], off) for p, off in zip((3, 4, 5), (0, 40, 72))]
    rows = a_hbm.shape[0]
    steps = rows // TILE

    def tile(i, size=TILE):
        return pl.ds(pl.multiple_of(i * size, size), size)

    def load_a(i):
        return pltpu.make_async_copy(a_hbm.at[tile(i, LOAD)], a_buf.at[tile(i, LOAD)], load_sem.at[i])

    load_b = pltpu.make_async_copy(b_hbm, b_buf, load_sem.at[rows // LOAD])
    for i in range(rows // LOAD):
        load_a(i).start()
    load_b.start()
    barrier = pltpu.get_barrier_semaphore()
    greet(barrier)
    acc[...] = jnp.zeros_like(acc)
    proj[...] = jnp.zeros_like(proj)

    @pl.loop(0, rows // WIDE)
    def _(i):
        for part in range(WIDE // LOAD):
            load_a(i * (WIDE // LOAD) + part).wait()
        a_lo = a_buf[tile(i, WIDE), :256]
        acc[:256, :256] += mm_t(a_lo, a_lo)
    pack(one[0].x, [block(acc, *ij) for ij in LOLO])

    @pl.loop(0, steps)
    def _(i):
        acc[:256, 256:] += mm_t(a_buf[tile(i), :256], a_buf[tile(i), 256:])

        @pl.when(i == 1)
        def _():
            pl.semaphore_wait(barrier, CHIPS)
            one[0].start()

        @pl.when(i == 2)
        def _():
            one[0].scatter()
    pack(one[1].x, [block(acc, *ij) for ij in LOHI])
    one[1].start()

    @pl.loop(0, steps)
    def _(i):
        a_hi = a_buf[tile(i), 256:]
        acc[256:, 256:] += mm_t(a_hi, a_hi)

        @pl.when(i == 0)
        def _():
            one[1].scatter()

        @pl.when(i == 2)
        def _():
            one[0].gather()
    pack(one[2].x, [block(acc, *ij) for ij in HIHI])
    one[2].start()
    one[2].scatter()
    one[1].gather()
    one[0].spread()
    factor(one, r_one, x_one, s_one, v_one)

    acc[...] = jnp.zeros_like(acc)
    load_b.wait()

    @pl.loop(0, rows // WIDE)
    def _(i):
        q_lo[tile(i, WIDE), :] = mm(a_buf[tile(i, WIDE), :256], x_one[:256, :256])

    @pl.loop(0, rows // WIDE)
    def _(i):
        q_blk = q_lo[tile(i, WIDE), :]
        acc[:256, :256] += mm_t(q_blk, q_blk)
        proj[:, :256] += mm_t(b_buf[tile(i, WIDE), :], q_blk)
    pack(two[0].x, [block(acc, *ij) for ij in LOLO] + [block(proj, 0, i) for i in range(2)])
    two[0].start()

    @pl.loop(0, rows // WIDE)
    def _(i):
        a_buf[tile(i, WIDE), 256:] = mm(a_buf[tile(i, WIDE), :], x_one[:, 256:])

        @pl.when(i == 0)
        def _():
            two[0].scatter()

    @pl.loop(0, rows // WIDE)
    def _(i):
        acc[:256, 256:] += mm_t(q_lo[tile(i, WIDE), :], a_buf[tile(i, WIDE), 256:])

        @pl.when(i == 0)
        def _():
            two[0].gather()
    pack(two[1].x, [block(acc, *ij) for ij in LOHI])
    two[1].start()

    @pl.loop(0, steps)
    def _(i):
        q_hi = a_buf[tile(i), 256:]
        acc[256:, 256:] += mm_t(q_hi, q_hi)
        proj[:, 256:] += mm_t(b_buf[tile(i), :], q_hi)

        @pl.when(i == 0)
        def _():
            two[1].scatter()

        @pl.when(i == 1)
        def _():
            two[0].spread()
    pack(two[2].x, [block(acc, *ij) for ij in HIHI] + [block(proj, 0, i) for i in range(2, 4)])
    two[2].start()
    two[2].scatter()
    two[1].gather()
    factor(two, r_two, x_two, s_two, v_two)

    sol[...] = mm(x_one[...], mm(x_two[...], r_two[:, 512:]))
    r_fac[:256, :256] = mm(r_two[:256, :256], r_one[:256, :256])
    r_fac[:256, 256:] = mm(r_two[:256, :512], r_one[:, 256:])
    r_fac[256:, 256:] = mm(r_two[256:, 256:512], r_one[256:, 256:])
    r_fac[256:, :256] = jnp.zeros((256, 256), jnp.float32)


def solution(mesh):
    def group_solve(a_blk, b_blk):
        rows = a_blk.shape[0]

        def buf(r, c=128):
            return pltpu.VMEM((r, c), jnp.float32)

        def piece(r):
            return [buf(r), buf(r), buf(r // 2), buf(r // 2), buf((CHIPS - 1) * CH), buf(CH), pltpu.SemaphoreType.DMA((8,))]
        return pl.pallas_call(
            solve_kernel,
            out_shape=(jax.ShapeDtypeStruct((512, 128), jnp.float32), jax.ShapeDtypeStruct((512, 512), jnp.float32)),
            in_specs=[pl.BlockSpec(memory_space=pl.ANY)] * 2,
            out_specs=(pl.BlockSpec(memory_space=pltpu.VMEM),) * 2,
            scratch_shapes=[buf(rows, 512), buf(rows, 256), buf(rows), buf(512, 512), buf(128, 512),
                            *piece(384), *piece(512), *piece(384), *piece(640), *piece(512), *piece(640),
                            buf(512, 512), buf(512), buf(512, 512), buf(512, 512),
                            buf(512, 640), buf(512), buf(512, 640), buf(512, 512),
                            pltpu.SemaphoreType.DMA((rows // LOAD + 1,))],
            compiler_params=pltpu.CompilerParams(collective_id=0, has_side_effects=True, vmem_limit_bytes=GIVE),
            name="solve",
        )(a_blk, b_blk)

    row_spec = P(("batch", "rows"), None)
    out_spec = P("batch", None)
    return jax.shard_map(group_solve, mesh=mesh, in_specs=(row_spec, row_spec), out_specs=(out_spec, out_spec), check_vma=False)
```

```python
import jax
import jax.numpy as jnp
from jax import lax
from jax.experimental import pallas as pl
from jax.experimental.pallas import tpu as pltpu
from jax.sharding import PartitionSpec as P

HIGHEST = lax.Precision.HIGHEST
CHIPS = 64
CH = 8
SPREAD, UNSPREAD = 27, 19
LOAD = 512
TILE = 1024
WIDE = 2048
GIVE = 60 * 1024 * 1024
LOLO = [(0, 0), (0, 1), (1, 1)]
LOHI = [(0, 2), (0, 3), (1, 2), (1, 3)]
HIHI = [(2, 2), (2, 3), (3, 3)]


def mm(a, b):
    return lax.dot_general(a, b, (((1,), (0,)), ((), ())), precision=HIGHEST, preferred_element_type=jnp.float32)


def mm_t(a, b):
    return lax.dot_general(a, b, (((0,), (0,)), ((), ())), precision=HIGHEST, preferred_element_type=jnp.float32)


def block(ref, j, i):
    return ref.at[j * 128:j * 128 + 128, i * 128:i * 128 + 128]


def place():
    dev = lax.axis_index("rows")
    return dev // 2, dev % 2


def greet(barrier):
    chip, core = place()
    pl.semaphore_signal(barrier, inc=1, device_id={"rows": chip * 2 + 1 - core})

    @pl.loop(1, CHIPS)
    def _(step):
        pl.semaphore_signal(barrier, inc=1, device_id={"rows": ((chip + step) % CHIPS) * 2 + core})


class Piece:
    def __init__(self, refs, offset):
        self.x, self.o, self.pair_buf, self.part, self.rs_buf, self.red, self.sems = refs
        self.offset = offset
        self.half = self.x.shape[0] // 2
        self.n_own = self.half // CH
        self.chip, self.core = place()
        self.mine = pl.multiple_of(self.core * self.half, CH)
        self.other = pl.multiple_of((1 - self.core) * self.half, CH)
        self.partner = {"rows": self.chip * 2 + 1 - self.core}
        self.idx = (self.chip * UNSPREAD + CHIPS - offset % CHIPS) % CHIPS
        self.owner = self.idx < self.n_own
        self.row = pl.multiple_of(self.idx * CH, CH)

    def swap_in(self):
        return pltpu.make_async_remote_copy(self.x.at[pl.ds(self.other, self.half)], self.pair_buf,
                                            self.sems.at[0], self.sems.at[1], device_id=self.partner)

    def swap_out(self):
        here = self.o.at[pl.ds(self.mine, self.half)]
        return pltpu.make_async_remote_copy(here, here, self.sems.at[6], self.sems.at[7], device_id=self.partner)

    def rows_of(self, n):
        return self.part.at[pl.ds(0, n * CH)]

    def start(self):
        self.swap_in().start()

    def scatter(self):
        self.swap_in().wait()
        self.part[...] = self.x[pl.ds(self.mine, self.half), :] + self.pair_buf[...]

        @pl.loop(0, self.n_own)
        def _(step):
            j = (step + self.chip) % self.n_own
            t = ((j + self.offset) * SPREAD) % CHIPS
            slot = (self.chip + CHIPS - t) % CHIPS - 1

            @pl.when(t != self.chip)
            def _():
                pltpu.make_async_remote_copy(self.part.at[pl.ds(pl.multiple_of(j * CH, CH), CH)],
                                             self.rs_buf.at[pl.ds(pl.multiple_of(slot * CH, CH), CH)],
                                             self.sems.at[2], self.sems.at[3], device_id={"rows": t * 2 + self.core}).start()

    def gather(self):
        @pl.when(self.owner)
        def _():
            pltpu.make_async_copy(self.rs_buf, self.rs_buf, self.sems.at[3]).wait()
            lanes = [self.part[pl.ds(self.row, CH), :]] + [self.rs_buf[s * CH:s * CH + CH, :] for s in range(CHIPS - 1)]
            while len(lanes) > 1:
                lanes = [u + v for u, v in zip(lanes[::2], lanes[1::2])]
            self.red[...] = lanes[0]
            self.o[pl.ds(self.mine + self.row, CH), :] = lanes[0]
            there = self.o.at[pl.ds(pl.multiple_of(self.mine + self.row, CH), CH)]

            @pl.loop(1, CHIPS)
            def _(step):
                pltpu.make_async_remote_copy(self.red, there, self.sems.at[4], self.sems.at[5],
                                             device_id={"rows": ((self.chip + step) % CHIPS) * 2 + self.core}).start()

    def spread(self):
        for own, n in ((True, self.n_own - 1), (False, self.n_own)):
            @pl.when(self.owner == own)
            def _():
                pltpu.make_async_copy(self.rows_of(n), self.rows_of(n), self.sems.at[5]).wait()
        self.swap_out().start()

    def finish(self):
        self.swap_out().wait()
        for own, n in ((True, self.n_own - 1), (False, self.n_own)):
            @pl.when(self.owner == own)
            def _():
                pltpu.make_async_copy(self.rows_of(n), self.rows_of(n), self.sems.at[2]).wait()

        @pl.when(self.owner)
        def _():
            pltpu.make_async_copy(self.rs_buf, self.rs_buf, self.sems.at[4]).wait()


def pack(ref, blocks):
    for t, blk in enumerate(blocks):
        ref[t * 128:t * 128 + 128, :] = blk[...]


def piece_block(ref, t):
    return ref[t * 128:t * 128 + 128, :]


def factor_block(d_mat):
    sub = lax.broadcasted_iota(jnp.int32, (8, 128), 0)
    lane = lax.broadcasted_iota(jnp.int32, (8, 128), 1)
    d_row = lax.broadcasted_iota(jnp.int32, (128, 128), 0)
    d_col = lax.broadcasted_iota(jnp.int32, (128, 128), 1)
    d_mat = jnp.where(d_col >= d_row, d_mat, d_mat.T)
    rows = [d_mat[8 * i:8 * i + 8, :] for i in range(16)]
    inv = [jnp.where(lane == sub + 8 * i, 1.0, 0.0).astype(jnp.float32) for i in range(16)]
    r_out, v_out = [], []
    for k in range(16):
        cols = {i: [jnp.broadcast_to(rows[i][:, 8 * k + r:8 * k + r + 1], (8, 128)) for r in range(8)] for i in range(k, 16)}
        scale = jnp.zeros((8, 128), jnp.float32)
        top = cols[k]
        for r in range(8):
            inv_root = lax.rsqrt(jnp.broadcast_to(top[r][r:r + 1, :], (8, 128)))
            scale = jnp.where(sub == r, inv_root, scale)
            below = jnp.where(sub > r, top[r] * inv_root, 0.0)
            row_s = jnp.broadcast_to(rows[k][r:r + 1, :], (8, 128)) * inv_root
            row_v = jnp.broadcast_to(inv[k][r:r + 1, :], (8, 128)) * inv_root
            coef = [jnp.broadcast_to(top[c][r:r + 1, :], (8, 128)) * inv_root for c in range(r + 1, 8)]
            for c in range(r + 1, 8):
                top[c] = top[c] - below * coef[c - r - 1]
            rows[k] = rows[k] - below * row_s
            inv[k] = inv[k] - below * row_v
            for i in range(k + 1, 16):
                mult = cols[i][r] * inv_root
                for c in range(r + 1, 8):
                    cols[i][c] = cols[i][c] - mult * coef[c - r - 1]
                rows[i] = rows[i] - mult * row_s
                inv[i] = inv[i] - mult * row_v
        r_out.append(jnp.where(lane >= sub + 8 * k, rows[k] * scale, 0.0))
        v_out.append(inv[k] * scale)
    return r_out, v_out


def factor(pieces, r_mat, x_out, s_mat, v_mat):
    width = s_mat.shape[1]
    p_lo, p_mid, p_hi = pieces
    s_mat[256:, 256:] = jnp.zeros((256, width - 256), jnp.float32)
    p_lo.finish()
    for t, (j, i) in enumerate(LOLO):
        block(s_mat, j, i)[...] = piece_block(p_lo.o, t)
    if width > 512:
        for t in range(2):
            block(s_mat, t, 4)[...] = piece_block(p_lo.o, 3 + t).T

    @pl.loop(0, 4)
    def _(j):
        top = pl.multiple_of(j * 128, 128)

        @pl.when(j == 2)
        def _():
            p_hi.finish()
            for t, (jj, ii) in enumerate(HIHI):
                block(s_mat, jj, ii)[...] += piece_block(p_hi.o, t)
            if width > 512:
                for t in range(2):
                    block(s_mat, 2 + t, 4)[...] += piece_block(p_hi.o, 3 + t).T
        r_blk, v_blk = factor_block(s_mat[pl.ds(top, 128), pl.ds(top, 128)])
        for i in range(16):
            r_mat[pl.ds(top + 8 * i, 8), pl.ds(top, 128)] = r_blk[i]
            v_mat[pl.ds(top + 8 * i, 8), :] = v_blk[i]

        @pl.when(j == 0)
        def _():
            p_mid.spread()
            p_hi.gather()
            p_mid.finish()
            for t, (jj, ii) in enumerate(LOHI):
                block(s_mat, jj, ii)[...] = piece_block(p_mid.o, t)

        @pl.when(j == 1)
        def _():
            p_hi.spread()
        for jj in range(4):
            lo, hi = 128 * jj, 128 * jj + 128
            if hi < width:
                @pl.when(j == jj)
                def _():
                    row = mm(v_mat[lo:hi, :], s_mat[lo:hi, hi:])
                    r_mat[lo:hi, hi:] = row
                    if hi < 512:
                        s_mat[hi:, hi:] = s_mat[hi:, hi:] - mm_t(row[:, :512 - hi], row)
    for jj in range(1, 4):
        r_mat[128 * jj:128 * jj + 128, :128 * jj] = jnp.zeros((128, 128 * jj), jnp.float32)
    for p in range(2):
        lo, mid, hi = 256 * p, 256 * p + 128, 256 * p + 256
        x_lo, x_hi = v_mat[lo:mid, :].T, v_mat[mid:hi, :].T
        x_out[lo:mid, lo:mid] = x_lo
        x_out[mid:hi, mid:hi] = x_hi
        x_out[mid:hi, lo:mid] = jnp.zeros((128, 128), jnp.float32)
        x_out[lo:mid, mid:hi] = -mm(x_lo, mm(r_mat[lo:mid, mid:hi], x_hi))
    x_out[256:, :256] = jnp.zeros((256, 256), jnp.float32)
    x_out[:256, 256:] = -mm(mm(x_out[:256, :256], r_mat[:256, 256:512]), x_out[256:, 256:])


def solve_kernel(a_hbm, b_hbm, sol, r_fac, a_buf, q_lo, b_buf, acc, proj, *refs):
    piece_refs, (s_one, v_one, r_one, x_one, s_two, v_two, r_two, x_two, load_sem) = refs[:42], refs[42:]
    one = [Piece(piece_refs[7 * p:7 * p + 7], off) for p, off in enumerate((0, 24, 56))]
    two = [Piece(piece_refs[7 * p:7 * p + 7], off) for p, off in zip((3, 4, 5), (0, 40, 72))]
    rows = a_hbm.shape[0]
    steps = rows // TILE

    def tile(i, size=TILE):
        return pl.ds(pl.multiple_of(i * size, size), size)

    def load_a(i):
        return pltpu.make_async_copy(a_hbm.at[tile(i, LOAD)], a_buf.at[tile(i, LOAD)], load_sem.at[i])

    load_b = pltpu.make_async_copy(b_hbm, b_buf, load_sem.at[rows // LOAD])
    for i in range(rows // LOAD):
        load_a(i).start()
    load_b.start()
    barrier = pltpu.get_barrier_semaphore()
    greet(barrier)
    acc[...] = jnp.zeros_like(acc)
    proj[...] = jnp.zeros_like(proj)

    @pl.loop(0, rows // WIDE)
    def _(i):
        for part in range(WIDE // LOAD):
            load_a(i * (WIDE // LOAD) + part).wait()
        a_lo = a_buf[tile(i, WIDE), :256]
        acc[:256, :256] += mm_t(a_lo, a_lo)
    pack(one[0].x, [block(acc, *ij) for ij in LOLO])
    pl.semaphore_wait(barrier, CHIPS)
    one[0].start()

    @pl.loop(0, steps)
    def _(i):
        acc[:256, 256:] += mm_t(a_buf[tile(i), :256], a_buf[tile(i), 256:])

        @pl.when(i == 0)
        def _():
            one[0].scatter()
    pack(one[1].x, [block(acc, *ij) for ij in LOHI])
    one[1].start()

    @pl.loop(0, steps)
    def _(i):
        a_hi = a_buf[tile(i), 256:]
        acc[256:, 256:] += mm_t(a_hi, a_hi)

        @pl.when(i == 0)
        def _():
            one[0].gather()
            one[1].scatter()
    pack(one[2].x, [block(acc, *ij) for ij in HIHI])
    one[2].start()
    one[0].spread()
    one[2].scatter()
    one[1].gather()
    factor(one, r_one, x_one, s_one, v_one)

    acc[...] = jnp.zeros_like(acc)
    load_b.wait()

    @pl.loop(0, rows // WIDE)
    def _(i):
        q_lo[tile(i, WIDE), :] = mm(a_buf[tile(i, WIDE), :256], x_one[:256, :256])

    @pl.loop(0, rows // WIDE)
    def _(i):
        q_blk = q_lo[tile(i, WIDE), :]
        acc[:256, :256] += mm_t(q_blk, q_blk)
        proj[:, :256] += mm_t(b_buf[tile(i, WIDE), :], q_blk)
    pack(two[0].x, [block(acc, *ij) for ij in LOLO] + [block(proj, 0, i) for i in range(2)])
    two[0].start()

    @pl.loop(0, steps)
    def _(i):
        a_buf[tile(i), 256:] = mm(a_buf[tile(i), :], x_one[:, 256:])

        @pl.when(i == 0)
        def _():
            two[0].scatter()

    @pl.loop(0, rows // WIDE)
    def _(i):
        acc[:256, 256:] += mm_t(q_lo[tile(i, WIDE), :], a_buf[tile(i, WIDE), 256:])

        @pl.when(i == 0)
        def _():
            two[0].gather()
    pack(two[1].x, [block(acc, *ij) for ij in LOHI])
    two[1].start()

    @pl.loop(0, steps)
    def _(i):
        q_hi = a_buf[tile(i), 256:]
        acc[256:, 256:] += mm_t(q_hi, q_hi)
        proj[:, 256:] += mm_t(b_buf[tile(i), :], q_hi)

        @pl.when(i == 0)
        def _():
            two[1].scatter()

        @pl.when(i == 2)
        def _():
            two[0].spread()
    pack(two[2].x, [block(acc, *ij) for ij in HIHI] + [block(proj, 0, i) for i in range(2, 4)])
    two[2].start()
    two[1].gather()
    two[2].scatter()
    factor(two, r_two, x_two, s_two, v_two)

    sol[...] = mm(x_one[...], mm(x_two[...], r_two[:, 512:]))
    r_fac[:256, :256] = mm(r_two[:256, :256], r_one[:256, :256])
    r_fac[:256, 256:] = mm(r_two[:256, :512], r_one[:, 256:])
    r_fac[256:, 256:] = mm(r_two[256:, 256:512], r_one[256:, 256:])
    r_fac[256:, :256] = jnp.zeros((256, 256), jnp.float32)


def hand_on(x_in, r_in, x_out, r_out, x_buf, r_buf, sems):
    copies = [pltpu.make_async_copy(*p, sems.at[i]) for i, p in enumerate(((x_in, x_buf), (r_in, r_buf), (x_buf, x_out), (r_buf, r_out)))]
    for c in copies[:2]:
        c.start()
    for i in range(2):
        copies[i].wait()
        copies[2 + i].start()
    for c in copies[2:]:
        c.wait()


def solution(mesh):
    def group_solve(a_blk, b_blk):
        rows = a_blk.shape[0]

        def buf(r, c=128):
            return pltpu.VMEM((r, c), jnp.float32)

        def piece(r):
            return [buf(r), buf(r), buf(r // 2), buf(r // 2), buf((CHIPS - 1) * CH), buf(CH), pltpu.SemaphoreType.DMA((8,))]
        results = pl.pallas_call(
            solve_kernel,
            out_shape=(jax.ShapeDtypeStruct((512, 128), jnp.float32), jax.ShapeDtypeStruct((512, 512), jnp.float32)),
            in_specs=[pl.BlockSpec(memory_space=pl.ANY)] * 2,
            out_specs=(pl.BlockSpec(memory_space=pltpu.VMEM),) * 2,
            scratch_shapes=[buf(rows, 512), buf(rows, 256), buf(rows), buf(512, 512), buf(128, 512),
                            *piece(384), *piece(512), *piece(384), *piece(640), *piece(512), *piece(640),
                            buf(512, 512), buf(512), buf(512, 512), buf(512, 512),
                            buf(512, 640), buf(512), buf(512, 640), buf(512, 512),
                            pltpu.SemaphoreType.DMA((rows // LOAD + 1,))],
            compiler_params=pltpu.CompilerParams(collective_id=0, has_side_effects=True, vmem_limit_bytes=GIVE),
            name="solve",
        )(a_blk, b_blk)
        return pl.pallas_call(
            hand_on,
            out_shape=tuple(jax.ShapeDtypeStruct(r.shape, r.dtype) for r in results),
            in_specs=[pl.BlockSpec(memory_space=pl.ANY)] * 2,
            out_specs=(pl.BlockSpec(memory_space=pl.ANY),) * 2,
            scratch_shapes=[pltpu.VMEM(r.shape, r.dtype) for r in results] + [pltpu.SemaphoreType.DMA((4,))],
            name="hand_on",
        )(*results)

    row_spec = P(("batch", "rows"), None)
    out_spec = P("batch", None)
    return jax.shard_map(group_solve, mesh=mesh, in_specs=(row_spec, row_spec), out_specs=(out_spec, out_spec), check_vma=False)
```

```python
import jax
import jax.numpy as jnp
from jax import lax
from jax.experimental import pallas as pl
from jax.experimental.pallas import tpu as pltpu
from jax.sharding import PartitionSpec as P

HIGHEST = lax.Precision.HIGHEST
CHIPS = 64
CH = 8
SPREAD, UNSPREAD = 27, 19
LOAD = 512
TILE = 1024
WIDE = 2048
GIVE = 60 * 1024 * 1024
LOLO = [(0, 0), (0, 1), (1, 1)]
LOHI = [(0, 2), (0, 3), (1, 2), (1, 3)]
HIHI = [(2, 2), (2, 3), (3, 3)]


def mm(a, b):
    return lax.dot_general(a, b, (((1,), (0,)), ((), ())), precision=HIGHEST, preferred_element_type=jnp.float32)


def mm_t(a, b):
    return lax.dot_general(a, b, (((0,), (0,)), ((), ())), precision=HIGHEST, preferred_element_type=jnp.float32)


def block(ref, j, i):
    return ref.at[j * 128:j * 128 + 128, i * 128:i * 128 + 128]


def place():
    dev = lax.axis_index("rows")
    return dev // 2, dev % 2


def greet(barrier):
    chip, core = place()
    pl.semaphore_signal(barrier, inc=1, device_id={"rows": chip * 2 + 1 - core})

    @pl.loop(1, CHIPS)
    def _(step):
        pl.semaphore_signal(barrier, inc=1, device_id={"rows": ((chip + step) % CHIPS) * 2 + core})


class Piece:
    def __init__(self, refs, offset):
        self.x, self.o, self.pair_buf, self.part, self.rs_buf, self.red, self.sems = refs
        self.offset = offset
        self.half = self.x.shape[0] // 2
        self.n_own = self.half // CH
        self.chip, self.core = place()
        self.mine = pl.multiple_of(self.core * self.half, CH)
        self.other = pl.multiple_of((1 - self.core) * self.half, CH)
        self.partner = {"rows": self.chip * 2 + 1 - self.core}
        self.idx = (self.chip * UNSPREAD + CHIPS - offset % CHIPS) % CHIPS
        self.owner = self.idx < self.n_own
        self.row = pl.multiple_of(self.idx * CH, CH)

    def swap_in(self):
        return pltpu.make_async_remote_copy(self.x.at[pl.ds(self.other, self.half)], self.pair_buf,
                                            self.sems.at[0], self.sems.at[1], device_id=self.partner)

    def swap_out(self):
        here = self.o.at[pl.ds(self.mine, self.half)]
        return pltpu.make_async_remote_copy(here, here, self.sems.at[6], self.sems.at[7], device_id=self.partner)

    def rows_of(self, n):
        return self.part.at[pl.ds(0, n * CH)]

    def start(self):
        self.swap_in().start()

    def scatter(self):
        self.swap_in().wait()
        self.part[...] = self.x[pl.ds(self.mine, self.half), :] + self.pair_buf[...]

        @pl.loop(0, self.n_own)
        def _(step):
            j = (step + self.chip) % self.n_own
            t = ((j + self.offset) * SPREAD) % CHIPS
            slot = (self.chip + CHIPS - t) % CHIPS - 1

            @pl.when(t != self.chip)
            def _():
                pltpu.make_async_remote_copy(self.part.at[pl.ds(pl.multiple_of(j * CH, CH), CH)],
                                             self.rs_buf.at[pl.ds(pl.multiple_of(slot * CH, CH), CH)],
                                             self.sems.at[2], self.sems.at[3], device_id={"rows": t * 2 + self.core}).start()

    def gather(self):
        @pl.when(self.owner)
        def _():
            pltpu.make_async_copy(self.rs_buf, self.rs_buf, self.sems.at[3]).wait()
            lanes = [self.part[pl.ds(self.row, CH), :]] + [self.rs_buf[s * CH:s * CH + CH, :] for s in range(CHIPS - 1)]
            while len(lanes) > 1:
                lanes = [u + v for u, v in zip(lanes[::2], lanes[1::2])]
            self.red[...] = lanes[0]
            self.o[pl.ds(self.mine + self.row, CH), :] = lanes[0]
            there = self.o.at[pl.ds(pl.multiple_of(self.mine + self.row, CH), CH)]

            @pl.loop(1, CHIPS)
            def _(step):
                pltpu.make_async_remote_copy(self.red, there, self.sems.at[4], self.sems.at[5],
                                             device_id={"rows": ((self.chip + step) % CHIPS) * 2 + self.core}).start()

    def spread(self):
        for own, n in ((True, self.n_own - 1), (False, self.n_own)):
            @pl.when(self.owner == own)
            def _():
                pltpu.make_async_copy(self.rows_of(n), self.rows_of(n), self.sems.at[5]).wait()
        self.swap_out().start()

    def finish(self):
        self.swap_out().wait()
        for own, n in ((True, self.n_own - 1), (False, self.n_own)):
            @pl.when(self.owner == own)
            def _():
                pltpu.make_async_copy(self.rows_of(n), self.rows_of(n), self.sems.at[2]).wait()

        @pl.when(self.owner)
        def _():
            pltpu.make_async_copy(self.rs_buf, self.rs_buf, self.sems.at[4]).wait()


def pack(ref, blocks):
    for t, blk in enumerate(blocks):
        ref[t * 128:t * 128 + 128, :] = blk[...]


def piece_block(ref, t):
    return ref[t * 128:t * 128 + 128, :]


def factor_block(d_mat):
    sub = lax.broadcasted_iota(jnp.int32, (8, 128), 0)
    lane = lax.broadcasted_iota(jnp.int32, (8, 128), 1)
    d_row = lax.broadcasted_iota(jnp.int32, (128, 128), 0)
    d_col = lax.broadcasted_iota(jnp.int32, (128, 128), 1)
    rows = jnp.where(d_col >= d_row, d_mat, d_mat.T).reshape(16, 8, 128)
    inv = jnp.where(d_col == d_row, 1.0, 0.0).astype(jnp.float32).reshape(16, 8, 128)

    def spread(v, r):
        return jnp.broadcast_to(v[r:r + 1, :], (8, 128))
    r_out, v_out = [], []
    for k in range(16):
        n = 15 - k
        row_k, inv_k = rows[0], inv[0]
        top = [jnp.broadcast_to(row_k[:, 8 * k + r:8 * k + r + 1], (8, 128)) for r in range(8)]
        if n:
            rows, inv = rows[1:], inv[1:]
            cols = [jnp.broadcast_to(rows[:, :, 8 * k + r:8 * k + r + 1], (n, 8, 128)) for r in range(8)]
        scale = jnp.zeros((8, 128), jnp.float32)
        for r in range(8):
            inv_root = lax.rsqrt(spread(top[r], r))
            scale = jnp.where(sub == r, inv_root, scale)
            below = jnp.where(sub > r, top[r] * inv_root, 0.0)
            row_s = spread(row_k, r) * inv_root
            row_v = spread(inv_k, r) * inv_root
            coef = [spread(top[c], r) * inv_root for c in range(r + 1, 8)]
            for c in range(r + 1, 8):
                top[c] = top[c] - below * coef[c - r - 1]
            row_k = row_k - below * row_s
            inv_k = inv_k - below * row_v
            if n:
                mult = cols[r] * inv_root
                for c in range(r + 1, 8):
                    cols[c] = cols[c] - mult * coef[c - r - 1]
                rows = rows - mult * row_s
                inv = inv - mult * row_v
        r_out.append(jnp.where(lane >= sub + 8 * k, row_k * scale, 0.0))
        v_out.append(inv_k * scale)
    return r_out, v_out


def factor(pieces, r_mat, x_out, s_mat, v_mat, beside, hooks):
    p_lo, p_mid, p_hi = pieces
    for jj in range(1, 4):
        r_mat[128 * jj:128 * jj + 128, :128 * jj] = jnp.zeros((128, 128 * jj), jnp.float32)
    x_out[256:, :256] = jnp.zeros((256, 256), jnp.float32)
    p_lo.finish()
    for t, ij in enumerate(LOLO):
        block(s_mat, *ij)[...] = piece_block(p_lo.o, t)

    for p in range(2):
        lo, mid, hi = 256 * p, 256 * p + 128, 256 * p + 256
        if p == 1:
            for t, ij in enumerate(LOHI):
                block(s_mat, *ij)[...] = piece_block(p_mid.o, t)
            right = mm_t(x_out[:256, :256], s_mat[:256, 256:])
            r_mat[:256, 256:] = right
            s_mat[256:, 256:] = mm_t(right, right)
            p_hi.finish()
            for t, ij in enumerate(HIHI):
                block(s_mat, *ij)[...] = piece_block(p_hi.o, t) - block(s_mat, *ij)[...]

        @pl.loop(0, 2)
        def _(j):
            top = pl.multiple_of(lo + j * 128, 128)
            r_blk, v_blk = factor_block(s_mat[pl.ds(top, 128), pl.ds(top, 128)])
            if p == 1:
                beside(j)
            for i in range(16):
                r_mat[pl.ds(top + 8 * i, 8), pl.ds(top, 128)] = r_blk[i]
                v_mat[pl.ds(top + 8 * i, 8), :] = v_blk[i]
            for jj in range(2):
                if (p, jj) in hooks:
                    pl.when(j == jj)(hooks[p, jj])

            @pl.when(j == 0)
            def _():
                row = mm(v_mat[lo:mid, :], s_mat[lo:mid, mid:hi])
                r_mat[lo:mid, mid:hi] = row
                s_mat[mid:hi, mid:hi] = s_mat[mid:hi, mid:hi] - mm_t(row, row)
        x_lo, x_hi = v_mat[lo:mid, :].T, v_mat[mid:hi, :].T
        x_out[lo:mid, lo:mid] = x_lo
        x_out[mid:hi, mid:hi] = x_hi
        x_out[mid:hi, lo:mid] = jnp.zeros((128, 128), jnp.float32)
        x_out[lo:mid, mid:hi] = -mm(x_lo, mm(r_mat[lo:mid, mid:hi], x_hi))
    x_out[:256, 256:] = -mm(mm(x_out[:256, :256], r_mat[:256, 256:]), x_out[256:, 256:])


def solve_kernel(a_hbm, b_hbm, sol, r_fac, a_buf, q_lo, b_buf, acc, proj, *refs):
    piece_refs, (s_one, v_one, r_one, x_one, s_two, v_two, r_two, x_two, load_sem) = refs[:49], refs[49:]
    one = [Piece(piece_refs[7 * p:7 * p + 7], off) for p, off in enumerate((0, 24, 56))]
    two = [Piece(piece_refs[7 * p:7 * p + 7], off) for p, off in zip((3, 4, 5, 6), (0, 24, 56, 16))]
    rows = a_hbm.shape[0]
    steps = rows // TILE

    def tile(i, size=TILE):
        return pl.ds(pl.multiple_of(i * size, size), size)

    def load_a(i):
        return pltpu.make_async_copy(a_hbm.at[tile(i, LOAD)], a_buf.at[tile(i, LOAD)], load_sem.at[i])

    load_b = pltpu.make_async_copy(b_hbm, b_buf, load_sem.at[rows // LOAD])
    for i in range(rows // LOAD):
        load_a(i).start()
    load_b.start()
    barrier = pltpu.get_barrier_semaphore()
    greet(barrier)
    acc[...] = jnp.zeros_like(acc)
    proj[...] = jnp.zeros_like(proj)

    @pl.loop(0, steps)
    def _(i):
        for part in range(TILE // LOAD):
            load_a(i * (TILE // LOAD) + part).wait()
        a_lo = a_buf[tile(i), :256]
        acc[:256, :256] += mm_t(a_lo, a_lo)
    pack(one[0].x, [block(acc, *ij) for ij in LOLO])
    pl.semaphore_wait(barrier, CHIPS)
    one[0].start()

    @pl.loop(0, steps)
    def _(i):
        acc[:256, 256:] += mm_t(a_buf[tile(i), :256], a_buf[tile(i), 256:])

        @pl.when(i == 0)
        def _():
            one[0].scatter()
    pack(one[1].x, [block(acc, *ij) for ij in LOHI])
    one[1].start()

    @pl.loop(0, steps)
    def _(i):
        a_hi = a_buf[tile(i), 256:]
        acc[256:, 256:] += mm_t(a_hi, a_hi)

        @pl.when(i == 0)
        def _():
            one[0].gather()
            one[1].scatter()
    pack(one[2].x, [block(acc, *ij) for ij in HIHI])
    one[2].start()
    one[2].scatter()
    one[1].gather()
    one[0].spread()

    def q_left(j):
        q_lo[tile(j, WIDE), :] = mm(a_buf[tile(j, WIDE), :256], x_one[:256, :256])

    def arrive(p_mid, p_hi):
        p_hi.gather()
        p_mid.spread()

    def arrived(p_mid, p_hi):
        p_mid.finish()
        p_hi.spread()
    factor(one, r_one, x_one, s_one, v_one, q_left,
           {(0, 0): lambda: arrive(one[1], one[2]), (0, 1): lambda: arrived(one[1], one[2])})

    acc[...] = jnp.zeros_like(acc)
    load_b.wait()

    @pl.loop(0, rows // WIDE)
    def _(i):
        q_blk = q_lo[tile(i, WIDE), :]
        acc[:256, :256] += mm_t(q_blk, q_blk)
    pack(two[0].x, [block(acc, *ij) for ij in LOLO])
    two[0].start()

    @pl.loop(0, steps)
    def _(i):
        a_buf[tile(i), 256:] = mm(a_buf[tile(i), :], x_one[:, 256:])

        @pl.when(i == 0)
        def _():
            two[0].scatter()

    @pl.loop(0, rows // WIDE)
    def _(i):
        acc[:256, 256:] += mm_t(q_lo[tile(i, WIDE), :], a_buf[tile(i, WIDE), 256:])

        @pl.when(i == 0)
        def _():
            two[0].gather()
    pack(two[1].x, [block(acc, *ij) for ij in LOHI])
    two[1].start()

    @pl.loop(0, steps)
    def _(i):
        q_hi = a_buf[tile(i), 256:]
        acc[256:, 256:] += mm_t(q_hi, q_hi)

        @pl.when(i == 0)
        def _():
            two[1].scatter()
    pack(two[2].x, [block(acc, *ij) for ij in HIHI])
    two[2].start()

    @pl.loop(0, steps)
    def _(i):
        b_blk = b_buf[tile(i), :]
        proj[:, :256] += mm_t(b_blk, q_lo[tile(i), :])
        proj[:, 256:] += mm_t(b_blk, a_buf[tile(i), 256:])

        @pl.when(i == 1)
        def _():
            two[2].scatter()
            two[0].spread()
    pack(two[3].x, [block(proj, 0, i) for i in range(4)])
    two[3].start()
    two[1].gather()

    def rows_of_r(j):
        at = pl.ds(pl.multiple_of(j * 128, 128), 128)
        r_fac[at, :] = mm(r_two[at, :], r_one[...])

    def arrive_two():
        arrive(two[1], two[2])
        two[3].scatter()

    def arrived_two():
        arrived(two[1], two[2])
        two[3].gather()
    factor(two[:3], r_two, x_two, s_two, v_two, rows_of_r, {(0, 0): arrive_two, (0, 1): arrived_two, (1, 0): two[3].spread})
    r_fac[256:, :256] = jnp.zeros((256, 256), jnp.float32)
    r_fac[256:, 256:] = mm(r_two[256:, 256:], r_one[256:, 256:])
    two[3].finish()
    for t in range(4):
        proj[:, t * 128:t * 128 + 128] = piece_block(two[3].o, t)
    sol[...] = mm(x_one[...], mm(x_two[...], mm(proj[...], x_two[...]).T))


def hand_on(x_in, r_in, x_out, r_out, x_buf, r_buf, sems):
    copies = [pltpu.make_async_copy(*p, sems.at[i]) for i, p in enumerate(((x_in, x_buf), (r_in, r_buf), (x_buf, x_out), (r_buf, r_out)))]
    for c in copies[:2]:
        c.start()
    for i in range(2):
        copies[i].wait()
        copies[2 + i].start()
    for c in copies[2:]:
        c.wait()


def solution(mesh):
    def group_solve(a_blk, b_blk):
        rows = a_blk.shape[0]

        def buf(r, c=128):
            return pltpu.VMEM((r, c), jnp.float32)

        def piece(r):
            return [buf(r), buf(r), buf(r // 2), buf(r // 2), buf((CHIPS - 1) * CH), buf(CH), pltpu.SemaphoreType.DMA((8,))]
        results = pl.pallas_call(
            solve_kernel,
            out_shape=(jax.ShapeDtypeStruct((512, 128), jnp.float32), jax.ShapeDtypeStruct((512, 512), jnp.float32)),
            in_specs=[pl.BlockSpec(memory_space=pl.ANY)] * 2,
            out_specs=(pl.BlockSpec(memory_space=pltpu.VMEM),) * 2,
            scratch_shapes=[buf(rows, 512), buf(rows, 256), buf(rows), buf(512, 512), buf(128, 512),
                            *piece(384), *piece(512), *piece(384), *piece(384), *piece(512), *piece(384), *piece(512),
                            buf(512, 512), buf(512), buf(512, 512), buf(512, 512),
                            buf(512, 512), buf(512), buf(512, 512), buf(512, 512),
                            pltpu.SemaphoreType.DMA((rows // LOAD + 1,))],
            compiler_params=pltpu.CompilerParams(collective_id=0, has_side_effects=True, vmem_limit_bytes=GIVE),
            name="solve",
        )(a_blk, b_blk)
        return pl.pallas_call(
            hand_on,
            out_shape=tuple(jax.ShapeDtypeStruct(r.shape, r.dtype) for r in results),
            in_specs=[pl.BlockSpec(memory_space=pl.ANY)] * 2,
            out_specs=(pl.BlockSpec(memory_space=pl.ANY),) * 2,
            scratch_shapes=[pltpu.VMEM(r.shape, r.dtype) for r in results] + [pltpu.SemaphoreType.DMA((4,))],
            name="hand_on",
        )(*results)

    row_spec = P(("batch", "rows"), None)
    out_spec = P("batch", None)
    return jax.shard_map(group_solve, mesh=mesh, in_specs=(row_spec, row_spec), out_specs=(out_spec, out_spec), check_vma=False)
```

```python
import jax
import jax.numpy as jnp
from jax import lax
from jax.experimental import pallas as pl
from jax.experimental.pallas import tpu as pltpu
from jax.sharding import PartitionSpec as P

HIGHEST = lax.Precision.HIGHEST
CHIPS = 64
CH = 8
SPREAD, UNSPREAD = 27, 19
LOAD = 512
TILE = 1024
WIDE = 2048
GIVE = 60 * 1024 * 1024
LOLO = [(0, 0), (0, 1), (1, 1)]
LOHI = [(0, 2), (0, 3), (1, 2), (1, 3)]
HIHI = [(2, 2), (2, 3), (3, 3)]


def mm(a, b):
    return lax.dot_general(a, b, (((1,), (0,)), ((), ())), precision=HIGHEST, preferred_element_type=jnp.float32)


def mm_t(a, b):
    return lax.dot_general(a, b, (((0,), (0,)), ((), ())), precision=HIGHEST, preferred_element_type=jnp.float32)


def block(ref, j, i):
    return ref.at[j * 128:j * 128 + 128, i * 128:i * 128 + 128]


def place():
    dev = lax.axis_index("rows")
    return dev // 2, dev % 2


def greet(barrier):
    chip, core = place()
    pl.semaphore_signal(barrier, inc=1, device_id={"rows": chip * 2 + 1 - core})

    @pl.loop(1, CHIPS)
    def _(step):
        pl.semaphore_signal(barrier, inc=1, device_id={"rows": ((chip + step) % CHIPS) * 2 + core})


class Piece:
    def __init__(self, refs, offset):
        self.x, self.o, self.pair_buf, self.part, self.rs_buf, self.red, self.sems = refs
        self.offset = offset
        self.half = self.x.shape[0] // 2
        self.n_own = self.half // CH
        self.chip, self.core = place()
        self.mine = pl.multiple_of(self.core * self.half, CH)
        self.other = pl.multiple_of((1 - self.core) * self.half, CH)
        self.partner = {"rows": self.chip * 2 + 1 - self.core}
        self.idx = (self.chip * UNSPREAD + CHIPS - offset % CHIPS) % CHIPS
        self.owner = self.idx < self.n_own
        self.row = pl.multiple_of(self.idx * CH, CH)

    def swap_in(self):
        return pltpu.make_async_remote_copy(self.x.at[pl.ds(self.other, self.half)], self.pair_buf,
                                            self.sems.at[0], self.sems.at[1], device_id=self.partner)

    def swap_out(self):
        here = self.o.at[pl.ds(self.mine, self.half)]
        return pltpu.make_async_remote_copy(here, here, self.sems.at[6], self.sems.at[7], device_id=self.partner)

    def rows_of(self, n):
        return self.part.at[pl.ds(0, n * CH)]

    def start(self):
        self.swap_in().start()

    def scatter(self):
        self.swap_in().wait()
        self.part[...] = self.x[pl.ds(self.mine, self.half), :] + self.pair_buf[...]

        @pl.loop(0, self.n_own)
        def _(step):
            j = (step + self.chip) % self.n_own
            t = ((j + self.offset) * SPREAD) % CHIPS
            slot = (self.chip + CHIPS - t) % CHIPS - 1

            @pl.when(t != self.chip)
            def _():
                pltpu.make_async_remote_copy(self.part.at[pl.ds(pl.multiple_of(j * CH, CH), CH)],
                                             self.rs_buf.at[pl.ds(pl.multiple_of(slot * CH, CH), CH)],
                                             self.sems.at[2], self.sems.at[3], device_id={"rows": t * 2 + self.core}).start()

    def gather(self):
        @pl.when(self.owner)
        def _():
            pltpu.make_async_copy(self.rs_buf, self.rs_buf, self.sems.at[3]).wait()
            lanes = [self.part[pl.ds(self.row, CH), :]] + [self.rs_buf[s * CH:s * CH + CH, :] for s in range(CHIPS - 1)]
            while len(lanes) > 1:
                lanes = [u + v for u, v in zip(lanes[::2], lanes[1::2])]
            self.red[...] = lanes[0]
            self.o[pl.ds(self.mine + self.row, CH), :] = lanes[0]
            there = self.o.at[pl.ds(pl.multiple_of(self.mine + self.row, CH), CH)]

            @pl.loop(1, CHIPS)
            def _(step):
                pltpu.make_async_remote_copy(self.red, there, self.sems.at[4], self.sems.at[5],
                                             device_id={"rows": ((self.chip + step) % CHIPS) * 2 + self.core}).start()

    def spread(self):
        for own, n in ((True, self.n_own - 1), (False, self.n_own)):
            @pl.when(self.owner == own)
            def _():
                pltpu.make_async_copy(self.rows_of(n), self.rows_of(n), self.sems.at[5]).wait()
        self.swap_out().start()

    def finish(self):
        self.swap_out().wait()
        for own, n in ((True, self.n_own - 1), (False, self.n_own)):
            @pl.when(self.owner == own)
            def _():
                pltpu.make_async_copy(self.rows_of(n), self.rows_of(n), self.sems.at[2]).wait()

        @pl.when(self.owner)
        def _():
            pltpu.make_async_copy(self.rs_buf, self.rs_buf, self.sems.at[4]).wait()


def pack(ref, blocks):
    for t, blk in enumerate(blocks):
        ref[t * 128:t * 128 + 128, :] = blk[...]


def piece_block(ref, t):
    return ref[t * 128:t * 128 + 128, :]


def factor_block(d_mat):
    sub = lax.broadcasted_iota(jnp.int32, (8, 128), 0)
    lane = lax.broadcasted_iota(jnp.int32, (8, 128), 1)
    d_row = lax.broadcasted_iota(jnp.int32, (128, 128), 0)
    d_col = lax.broadcasted_iota(jnp.int32, (128, 128), 1)
    rows = jnp.where(d_col >= d_row, d_mat, d_mat.T).reshape(16, 8, 128)
    inv = jnp.where(d_col == d_row, 1.0, 0.0).astype(jnp.float32).reshape(16, 8, 128)

    def spread(v, r):
        return jnp.broadcast_to(v[r:r + 1, :], (8, 128))
    r_out, v_out = [], []
    for k in range(16):
        n = 15 - k
        row_k, inv_k = rows[0], inv[0]
        top = [jnp.broadcast_to(row_k[:, 8 * k + r:8 * k + r + 1], (8, 128)) for r in range(8)]
        if n:
            rows, inv = rows[1:], inv[1:]
            cols = [jnp.broadcast_to(rows[:, :, 8 * k + r:8 * k + r + 1], (n, 8, 128)) for r in range(8)]
        scale = jnp.zeros((8, 128), jnp.float32)
        for r in range(8):
            inv_root = lax.rsqrt(spread(top[r], r))
            scale = jnp.where(sub == r, inv_root, scale)
            below = jnp.where(sub > r, top[r] * inv_root, 0.0)
            row_s = spread(row_k, r) * inv_root
            row_v = spread(inv_k, r) * inv_root
            coef = [spread(top[c], r) * inv_root for c in range(r + 1, 8)]
            for c in range(r + 1, 8):
                top[c] = top[c] - below * coef[c - r - 1]
            row_k = row_k - below * row_s
            inv_k = inv_k - below * row_v
            if n:
                mult = cols[r] * inv_root
                for c in range(r + 1, 8):
                    cols[c] = cols[c] - mult * coef[c - r - 1]
                rows = rows - mult * row_s
                inv = inv - mult * row_v
        r_out.append(jnp.where(lane >= sub + 8 * k, row_k * scale, 0.0))
        v_out.append(inv_k * scale)
    return r_out, v_out


def factor(pieces, r_mat, x_out, s_mat, v_mat, beside, hooks):
    p_lo, p_mid, p_hi = pieces
    for jj in range(1, 4):
        r_mat[128 * jj:128 * jj + 128, :128 * jj] = jnp.zeros((128, 128 * jj), jnp.float32)
    x_out[256:, :256] = jnp.zeros((256, 256), jnp.float32)
    p_lo.finish()
    for t, ij in enumerate(LOLO):
        block(s_mat, *ij)[...] = piece_block(p_lo.o, t)

    for p in range(2):
        lo, mid, hi = 256 * p, 256 * p + 128, 256 * p + 256
        if p == 1:
            for t, ij in enumerate(LOHI):
                block(s_mat, *ij)[...] = piece_block(p_mid.o, t)
            right = mm_t(x_out[:256, :256], s_mat[:256, 256:])
            r_mat[:256, 256:] = right
            s_mat[256:, 256:] = mm_t(right, right)
            p_hi.finish()
            for t, ij in enumerate(HIHI):
                block(s_mat, *ij)[...] = piece_block(p_hi.o, t) - block(s_mat, *ij)[...]

        @pl.loop(0, 2)
        def _(j):
            top = pl.multiple_of(lo + j * 128, 128)
            r_blk, v_blk = factor_block(s_mat[pl.ds(top, 128), pl.ds(top, 128)])
            if p == 1:
                beside(j)
                s_mat[:256, :256] = mm(x_out[:256, :256], r_mat[:256, 256:])
            for i in range(16):
                r_mat[pl.ds(top + 8 * i, 8), pl.ds(top, 128)] = r_blk[i]
                v_mat[pl.ds(top + 8 * i, 8), :] = v_blk[i]
            for jj in range(2):
                if (p, jj) in hooks:
                    pl.when(j == jj)(hooks[p, jj])

            @pl.when(j == 0)
            def _():
                row = mm(v_mat[lo:mid, :], s_mat[lo:mid, mid:hi])
                r_mat[lo:mid, mid:hi] = row
                s_mat[mid:hi, mid:hi] = s_mat[mid:hi, mid:hi] - mm_t(row, row)
        x_lo, x_hi = v_mat[lo:mid, :].T, v_mat[mid:hi, :].T
        x_out[lo:mid, lo:mid] = x_lo
        x_out[mid:hi, mid:hi] = x_hi
        x_out[mid:hi, lo:mid] = jnp.zeros((128, 128), jnp.float32)
        x_out[lo:mid, mid:hi] = -mm(x_lo, mm(r_mat[lo:mid, mid:hi], x_hi))
    x_out[:256, 256:] = -mm(s_mat[:256, :256], x_out[256:, 256:])


def solve_kernel(a_hbm, b_hbm, sol, r_fac, a_buf, q_lo, b_buf, acc, proj, *refs):
    piece_refs, (s_one, v_one, r_one, x_one, s_two, v_two, r_two, x_two, load_sem) = refs[:49], refs[49:]
    one = [Piece(piece_refs[7 * p:7 * p + 7], off) for p, off in enumerate((0, 24, 56))]
    two = [Piece(piece_refs[7 * p:7 * p + 7], off) for p, off in zip((3, 4, 5, 6), (0, 24, 56, 16))]
    rows = a_hbm.shape[0]
    steps = rows // TILE

    def tile(i, size=TILE):
        return pl.ds(pl.multiple_of(i * size, size), size)

    def load_a(i):
        return pltpu.make_async_copy(a_hbm.at[tile(i, LOAD)], a_buf.at[tile(i, LOAD)], load_sem.at[i])

    load_b = pltpu.make_async_copy(b_hbm, b_buf, load_sem.at[rows // LOAD])
    for i in range(rows // LOAD):
        load_a(i).start()
    load_b.start()
    barrier = pltpu.get_barrier_semaphore()
    greet(barrier)
    acc[...] = jnp.zeros_like(acc)
    proj[...] = jnp.zeros_like(proj)

    @pl.loop(0, steps)
    def _(i):
        for part in range(TILE // LOAD):
            load_a(i * (TILE // LOAD) + part).wait()
        a_lo = a_buf[tile(i), :256]
        acc[:256, :256] += mm_t(a_lo, a_lo)
    pack(one[0].x, [block(acc, *ij) for ij in LOLO])
    pl.semaphore_wait(barrier, CHIPS)
    one[0].start()

    @pl.loop(0, steps)
    def _(i):
        acc[:256, 256:] += mm_t(a_buf[tile(i), :256], a_buf[tile(i), 256:])

        @pl.when(i == 0)
        def _():
            one[0].scatter()
    pack(one[1].x, [block(acc, *ij) for ij in LOHI])
    one[1].start()

    @pl.loop(0, steps)
    def _(i):
        a_hi = a_buf[tile(i), 256:]
        acc[256:, 256:] += mm_t(a_hi, a_hi)

        @pl.when(i == 0)
        def _():
            one[0].gather()
            one[1].scatter()
    pack(one[2].x, [block(acc, *ij) for ij in HIHI])
    one[2].start()
    one[2].scatter()
    one[0].spread()
    one[1].gather()

    def q_left(j):
        q_lo[tile(j, WIDE), :] = mm(a_buf[tile(j, WIDE), :256], x_one[:256, :256])

    def arrive(p_mid, p_hi):
        p_hi.gather()
        p_mid.spread()

    def arrived(p_mid, p_hi):
        p_mid.finish()
        p_hi.spread()
    factor(one, r_one, x_one, s_one, v_one, q_left,
           {(0, 0): lambda: arrive(one[1], one[2]), (0, 1): lambda: arrived(one[1], one[2])})

    acc[...] = jnp.zeros_like(acc)
    load_b.wait()

    @pl.loop(0, rows // WIDE)
    def _(i):
        q_blk = q_lo[tile(i, WIDE), :]
        acc[:256, :256] += mm_t(q_blk, q_blk)
    pack(two[0].x, [block(acc, *ij) for ij in LOLO])
    two[0].start()

    @pl.loop(0, steps)
    def _(i):
        a_buf[tile(i), 256:] = mm(a_buf[tile(i), :], x_one[:, 256:])

        @pl.when(i == 0)
        def _():
            two[0].scatter()

    @pl.loop(0, rows // WIDE)
    def _(i):
        acc[:256, 256:] += mm_t(q_lo[tile(i, WIDE), :], a_buf[tile(i, WIDE), 256:])

        @pl.when(i == 0)
        def _():
            two[0].gather()
    pack(two[1].x, [block(acc, *ij) for ij in LOHI])
    two[1].start()

    @pl.loop(0, steps)
    def _(i):
        q_hi = a_buf[tile(i), 256:]
        acc[256:, 256:] += mm_t(q_hi, q_hi)

        @pl.when(i == 0)
        def _():
            two[1].scatter()
    pack(two[2].x, [block(acc, *ij) for ij in HIHI])
    two[2].start()

    @pl.loop(0, steps)
    def _(i):
        b_blk = b_buf[tile(i), :]
        proj[:, :256] += mm_t(b_blk, q_lo[tile(i), :])
        proj[:, 256:] += mm_t(b_blk, a_buf[tile(i), 256:])

        @pl.when(i == 1)
        def _():
            two[2].scatter()
            two[0].spread()
    pack(two[3].x, [block(proj, 0, i) for i in range(4)])
    two[3].start()
    two[1].gather()

    def rows_of_r(j):
        at = pl.ds(pl.multiple_of(j * 128, 128), 128)
        r_fac[at, :] = mm(r_two[at, :], r_one[...])

    def arrive_two():
        arrive(two[1], two[2])
        two[3].scatter()

    def arrived_two():
        arrived(two[1], two[2])
        two[3].gather()
    factor(two[:3], r_two, x_two, s_two, v_two, rows_of_r, {(0, 0): arrive_two, (0, 1): arrived_two, (1, 0): two[3].spread})
    r_fac[256:, :256] = jnp.zeros((256, 256), jnp.float32)
    r_fac[256:, 256:] = mm(r_two[256:, 256:], r_one[256:, 256:])
    two[3].finish()
    for t in range(4):
        proj[:, t * 128:t * 128 + 128] = piece_block(two[3].o, t)
    sol[...] = mm(x_one[...], mm(x_two[...], mm(proj[...], x_two[...]).T))


def hand_on(x_in, r_in, x_out, r_out, x_buf, r_buf, sems):
    copies = [pltpu.make_async_copy(*p, sems.at[i]) for i, p in enumerate(((x_in, x_buf), (r_in, r_buf), (x_buf, x_out), (r_buf, r_out)))]
    for c in copies[:2]:
        c.start()
    for i in range(2):
        copies[i].wait()
        copies[2 + i].start()
    for c in copies[2:]:
        c.wait()


def solution(mesh):
    def group_solve(a_blk, b_blk):
        rows = a_blk.shape[0]

        def buf(r, c=128):
            return pltpu.VMEM((r, c), jnp.float32)

        def piece(r):
            return [buf(r), buf(r), buf(r // 2), buf(r // 2), buf((CHIPS - 1) * CH), buf(CH), pltpu.SemaphoreType.DMA((8,))]
        results = pl.pallas_call(
            solve_kernel,
            out_shape=(jax.ShapeDtypeStruct((512, 128), jnp.float32), jax.ShapeDtypeStruct((512, 512), jnp.float32)),
            in_specs=[pl.BlockSpec(memory_space=pl.ANY)] * 2,
            out_specs=(pl.BlockSpec(memory_space=pltpu.VMEM),) * 2,
            scratch_shapes=[buf(rows, 512), buf(rows, 256), buf(rows), buf(512, 512), buf(128, 512),
                            *piece(384), *piece(512), *piece(384), *piece(384), *piece(512), *piece(384), *piece(512),
                            buf(512, 512), buf(512), buf(512, 512), buf(512, 512),
                            buf(512, 512), buf(512), buf(512, 512), buf(512, 512),
                            pltpu.SemaphoreType.DMA((rows // LOAD + 1,))],
            compiler_params=pltpu.CompilerParams(collective_id=0, has_side_effects=True, vmem_limit_bytes=GIVE),
            name="solve",
        )(a_blk, b_blk)
        return pl.pallas_call(
            hand_on,
            out_shape=tuple(jax.ShapeDtypeStruct(r.shape, r.dtype) for r in results),
            in_specs=[pl.BlockSpec(memory_space=pl.ANY)] * 2,
            out_specs=(pl.BlockSpec(memory_space=pl.ANY),) * 2,
            scratch_shapes=[pltpu.VMEM(r.shape, r.dtype) for r in results] + [pltpu.SemaphoreType.DMA((4,))],
            name="hand_on",
        )(*results)

    row_spec = P(("batch", "rows"), None)
    out_spec = P("batch", None)
    return jax.shard_map(group_solve, mesh=mesh, in_specs=(row_spec, row_spec), out_specs=(out_spec, out_spec), check_vma=False)
```
